32 devices in a mesh: seq: 8 (over y, x, core), dp: 4 (over z).
Axes of the slice: x: 2, y: 2, z: 4, core: 2. Of those that a mesh axis runs over, the one named last changes fastest.
Arguments:
- normed_input: bfloat16 [4, 1024, 2304], P('dp', 'seq'), may hold values from -6 to 6
- queries: bfloat16 [4, 1024, 2048], P('dp', 'seq'), may hold values from -9 to 9
- rotated_key_states: bfloat16 [4, 1024, 1024], P('dp', 'seq'), may hold values from -9 to 9
- value_head_states: bfloat16 [4, 1024, 1024], P('dp', 'seq'), may hold values from -6 to 6
- saved_attention_output: bfloat16 [4, 1024, 2048], P('dp', 'seq'), may hold values from -6 to 6
- output_cotangent: bfloat16 [4, 1024, 2048], P('dp', 'seq'), may hold values from -6 to 6
- doc_ids: int32 [4, 1024], P('dp', 'seq'), may hold values from 0 to 7, never falling along the last dimension, each value on 1 to 512 neighbouring positions
Outputs:
- query_grad: bfloat16 [4, 1024, 2048], P('dp', 'seq')
- key_grad: bfloat16 [4, 1024, 1024], P('dp', 'seq')
- value_weight_grad: float32 [2304, 1024], P(('seq', 'dp'))
The draws below stay inside these ranges and needn't reach their ends.
Inputs may be any that keep to these rules, and one draw needn't show every extreme that they name: `doc_ids`: within each sequence document ids never fall; each document holds 1 to 512 positions.
All inputs are finite; a program needn't handle non-finite values.
Results may differ from the reference program's by a relative error of at most 0.009.
Values may be sent and summed in bfloat16 or wider, within the bound.
A program may use at most 128 MiB of HBM per device.

```python
import math
import jax
import jax.numpy as jnp
import numpy as np
from jax import lax

QUERY_HEADS = 16
KEY_VALUE_HEADS = 8
HEAD_WIDTH = 128
DWIN = 2304
TOKENS_PER_SHARD = 128
SEQUENCE_LENGTH = 1024
BATCH_COUNT = 4
N_SEQ = 8


def level_of(rng, dims, pieces, low, high):
    level, own = 1.0, jax.random.fold_in(rng, 6)
    for dim, parts in pieces:
        heights = jnp.exp(jax.random.uniform(jax.random.fold_in(own, dim), (parts,), jnp.float32, low / len(pieces), high / len(pieces)))
        level = level * jnp.repeat(heights, dims[dim] // parts).reshape([-1 if axis == dim else 1 for axis in range(len(dims))])
    return level


def profile(count, total, limit, lean):
    loads = [(1 << 20) // math.isqrt(grade ** lean) + 1 for grade in range(2, count + 1)]
    spare, holding = total - limit - (count - 1), [1] * (count - 1)
    while spare > 0:
        movable = [i for i in range(count - 1) if holding[i] < limit]
        whole, budget = sum([loads[i] for i in movable]), spare
        for i in movable:
            addition = min(limit - holding[i], max(1, budget * loads[i] // whole), spare)
            holding[i] = holding[i] + addition
            spare = spare - addition
    return np.array([limit] + holding)


def ragged(own_key, amount, total, reach, slope):
    if amount == 2:
        one = jax.random.randint(own_key, (), max(1, total - reach), min(reach, total - 1) + 1)
        return jnp.stack([one, total - one])
    lengths = jnp.asarray(profile(amount, total, reach, slope), jnp.int32)
    couples = (amount - 1) // 2
    donor, taker = lengths[1:1 + 2 * couples:2], lengths[2:2 + 2 * couples:2]
    slack = jnp.minimum(donor - 1, reach - taker)
    shifted = jax.random.randint(jax.random.fold_in(own_key, 1), (couples,), 0, 1 << 20) % (slack + 1)
    lengths = lengths.at[1:1 + 2 * couples:2].set(donor - shifted).at[2:2 + 2 * couples:2].set(taker + shifted)
    return lengths[jax.random.permutation(jax.random.fold_in(own_key, 2), amount)]


def normal_values(stream_key, dims, spread, reach, shards=(), kind=jnp.bfloat16):
    loudness = level_of(stream_key, dims, shards, -0.22, 0.18) if shards else 1.0
    entries = jax.random.normal(stream_key, dims, jnp.float32) * spread * loudness
    return jnp.minimum(jnp.maximum(entries, -reach), reach).astype(kind)


def setup_inputs(seed: int = 0) -> dict:
    splits = jax.random.split(jax.random.key(seed), 8)
    normed_input = normal_values(splits[0], (BATCH_COUNT, SEQUENCE_LENGTH, DWIN), 1.0, 6.0, ((0, 4), (1, 8)))
    queries = normal_values(splits[1], (BATCH_COUNT, SEQUENCE_LENGTH, QUERY_HEADS * HEAD_WIDTH), 1.5, 9.0, ((0, 4), (1, 8)))
    rotated_key_states = normal_values(splits[2], (BATCH_COUNT, SEQUENCE_LENGTH, KEY_VALUE_HEADS * HEAD_WIDTH), 1.5, 9.0, ((0, 4), (1, 8)))
    value_head_states = normal_values(splits[3], (BATCH_COUNT, SEQUENCE_LENGTH, KEY_VALUE_HEADS * HEAD_WIDTH), 1.0, 6.0, ((0, 4), (1, 8)))
    saved_attention_output = normal_values(splits[4], (BATCH_COUNT, SEQUENCE_LENGTH, QUERY_HEADS * HEAD_WIDTH), 1.0, 6.0, ((0, 4), (1, 8)))
    output_cotangent = normal_values(splits[5], (BATCH_COUNT, SEQUENCE_LENGTH, QUERY_HEADS * HEAD_WIDTH), 1.0, 6.0, ((0, 4), (1, 8)))
    doc_ids = jax.vmap(lambda own: jnp.searchsorted(jnp.cumsum(ragged(own, 8, SEQUENCE_LENGTH, SEQUENCE_LENGTH // 2, 1)), jnp.arange(SEQUENCE_LENGTH), side="right"))(jax.random.split(splits[6], BATCH_COUNT)).reshape((BATCH_COUNT, SEQUENCE_LENGTH)).astype(jnp.int32)
    return {"normed_input": normed_input, "queries": queries, "rotated_key_states": rotated_key_states, "value_head_states": value_head_states, "saved_attention_output": saved_attention_output, "output_cotangent": output_cotangent, "doc_ids": doc_ids}


query_scale = 144.0 ** -0.5
soft_cap = 50.0


def reference(normed_input, queries, rotated_key_states, value_head_states, saved_attention_output, output_cotangent, doc_ids):
    query_groups = QUERY_HEADS // KEY_VALUE_HEADS
    key_value_width = KEY_VALUE_HEADS * HEAD_WIDTH
    positions = jnp.arange(SEQUENCE_LENGTH, dtype=jnp.int32)

    def one_sequence(weight_total, items):
        inputs_row, gathered_queries, gathered_keys, gathered_values, gathered_outputs, gathered_gradients, docs_all = items
        key_row_block = gathered_keys.reshape(SEQUENCE_LENGTH, KEY_VALUE_HEADS, HEAD_WIDTH).astype(jnp.float32)
        value_row_block = gathered_values.reshape(SEQUENCE_LENGTH, KEY_VALUE_HEADS, HEAD_WIDTH).astype(jnp.float32)

        def one_shard(running, number):
            leading_row = (number * TOKENS_PER_SHARD).astype(jnp.int32)
            query_row_block = lax.dynamic_slice_in_dim(gathered_queries, leading_row, TOKENS_PER_SHARD, 0).reshape(TOKENS_PER_SHARD, KEY_VALUE_HEADS, query_groups, HEAD_WIDTH)
            output_gradients = lax.dynamic_slice_in_dim(gathered_gradients, leading_row, TOKENS_PER_SHARD, 0).reshape(TOKENS_PER_SHARD, KEY_VALUE_HEADS, query_groups, HEAD_WIDTH)
            output_result = lax.dynamic_slice_in_dim(gathered_outputs, leading_row, TOKENS_PER_SHARD, 0).reshape(TOKENS_PER_SHARD, KEY_VALUE_HEADS, query_groups, HEAD_WIDTH)
            query_doc = lax.dynamic_slice_in_dim(docs_all, leading_row, TOKENS_PER_SHARD, 0)
            query_pos = lax.dynamic_slice_in_dim(positions, leading_row, TOKENS_PER_SHARD, 0)
            query_wide = query_row_block.astype(jnp.float32)
            grads_wide = output_gradients.astype(jnp.float32)
            deltas = jnp.einsum("qhgd,qhgd->hgq", grads_wide, output_result.astype(jnp.float32))
            raw_scores = jnp.einsum("qhgd,khd->hgqk", query_wide, key_row_block)
            capped = soft_cap * jnp.tanh(raw_scores * (query_scale / soft_cap))
            allowed = (positions[None, :] <= query_pos[:, None]) & (docs_all[None, :] == query_doc[:, None])
            weights = jnp.where(allowed, jnp.exp(capped), 0.0)
            totals = jnp.sum(weights, axis=-1)
            probabilities = weights / totals[..., None]
            prob_grads = jnp.einsum("qhgd,khd->hgqk", grads_wide, value_row_block)
            score_grads = probabilities * (prob_grads - deltas[..., None]) * (1.0 - (capped / soft_cap) ** 2) * query_scale
            score_rounded = score_grads.astype(jnp.bfloat16).astype(jnp.float32)
            prob_rounded = probabilities.astype(jnp.bfloat16).astype(jnp.float32)
            query_part = jnp.einsum("hgqk,khd->qhgd", score_rounded, key_row_block)
            key_part = jnp.einsum("hgqk,qhgd->khd", score_rounded, query_wide).reshape(SEQUENCE_LENGTH, key_value_width)
            value_part = jnp.einsum("hgqk,qhgd->khd", prob_rounded, grads_wide).reshape(SEQUENCE_LENGTH, key_value_width)
            kv_terms = jnp.concatenate([key_part, value_part], axis=1).astype(jnp.bfloat16)
            query_out = query_part.reshape(TOKENS_PER_SHARD, QUERY_HEADS * HEAD_WIDTH).astype(jnp.bfloat16)
            return running + kv_terms.astype(jnp.float32), query_out

        start_sum = jnp.zeros((SEQUENCE_LENGTH, 2 * key_value_width), jnp.float32)
        summed, query_parts = lax.scan(one_shard, start_sum, jnp.arange(N_SEQ, dtype=jnp.int32))
        query_grad = query_parts.reshape(SEQUENCE_LENGTH, QUERY_HEADS * HEAD_WIDTH)
        key_grad = summed[:, :key_value_width].astype(jnp.bfloat16)
        value_grad = summed[:, key_value_width:].astype(jnp.bfloat16)
        weight_term = jnp.dot(inputs_row.T, value_grad, preferred_element_type=jnp.float32)
        return weight_total + weight_term, (query_grad, key_grad)

    start_weight = jnp.zeros((DWIN, key_value_width), jnp.float32)
    weight_total, (query_grad, key_grad) = lax.scan(one_sequence, start_weight, (normed_input, queries, rotated_key_states, value_head_states, saved_attention_output, output_cotangent, doc_ids))
    value_weight_grad = weight_total * ((BATCH_COUNT * SEQUENCE_LENGTH) ** -0.5)
    return query_grad, key_grad, value_weight_grad
```

```python
import functools

import jax
import jax.numpy as jnp
from jax import lax
from jax.experimental import pallas as pl
from jax.experimental.pallas import tpu as pltpu
from jax.sharding import PartitionSpec as P

QUERY_HEADS = 16
KEY_VALUE_HEADS = 8
HEAD_WIDTH = 128
CORES = 2
MESH = pl.DeviceIdType.MESH

query_scale = 144.0 ** (-0.5)
soft_cap = 50.0


def flip(index, mask, count):
    out, bit = 0, 1
    while bit < count:
        digit = lax.rem(index // bit, 2)
        out = out + (1 - digit if mask & bit else digit) * bit
        bit *= 2
    return out


def at(index, width):
    start = index * width
    return pl.ds(start if isinstance(index, int) else pl.multiple_of(start, width), width)


def nt(a, b):
    return lax.dot_general(a, b, (((1,), (1,)), ((), ())), preferred_element_type=jnp.float32)


def tn(a, b):
    return lax.dot_general(a, b, (((0,), (0,)), ((), ())), preferred_element_type=jnp.float32)


def kernel(
    n, ndp, total_tokens,
    x_in, q_in, k_in, v_in, o_in, do_in, doc_in,
    dq_out, dk_out, dw_out,
    x_ref, q_ref, k_ref, v_ref, o_ref, do_ref, doc_ref,
    rq, rk, rv, rdo, meta, rmeta, xt, rx, dock,
    dk_acc, dv_acc, dqs, dks, rdk, vg, pf, zs, zr,
    load_sem, in_send, in_recv, local_sem, dq_send, dq_recv, dk_send, dk_recv, vg_send, vg_recv,
    relay_send, relay_recv, fwd_send, fwd_recv, z_send, z_recv,
):
    me = lax.axis_index("seq")
    dme = lax.axis_index("dp")
    tokens = q_ref.shape[0]
    seq = n * tokens
    hw = HEAD_WIDTH
    group = QUERY_HEADS // KEY_VALUE_HEADS
    hq = QUERY_HEADS // n
    copies = group // hq
    rows = x_ref.shape[1] // n
    piece = rows // ndp
    chips = n // CORES
    width = CORES * hw // copies
    reach = (seq // 2 - 1 + tokens - 1) // tokens
    chip, core = me // CORES, lax.rem(me, CORES)
    partner = chip * CORES + (1 - core)

    barrier = pltpu.get_barrier_semaphore()
    for off in range(1, ndp):
        pl.semaphore_signal(
            barrier, inc=1, device_id={"dp": lax.rem(dme + off, ndp)}, device_id_type=MESH
        )
    for off in range(n - 1, 0, -1):
        pl.semaphore_signal(barrier, inc=1, device_id={"seq": flip(me, off, n)}, device_id_type=MESH)

    loads = [
        pltpu.make_async_copy(src, dst, load_sem.at[index])
        for index, (src, dst) in enumerate((
            (do_in, do_ref), (o_in, o_ref), (doc_in, doc_ref), (x_in, x_ref),
            (k_in, k_ref), (v_in, v_ref), (q_in, q_ref),
        ))
    ]
    for load in loads:
        load.start()

    def inputs(dest, slot, local=False):
        kv = dest * hq // group
        sources = (k_in, v_in, q_in, do_in) if local else (k_ref, v_ref, q_ref, do_ref)
        return [
            (sources[0].at[:, at(kv, hw)], rk.at[at(slot, tokens), :]),
            (sources[1].at[:, at(kv, hw)], rv.at[at(slot, tokens), :]),
            (sources[2].at[:, at(dest, hq * hw)], rq.at[at(slot, tokens), :]),
            (sources[3].at[:, at(dest, hq * hw)], rdo.at[at(slot, tokens), :]),
            (meta.at[dest], rmeta.at[slot]),
            (xt.at[at(dest, rows), :], rx.at[:, at(slot, tokens)]),
        ]

    def input_copy(kind, off):
        peer = flip(me, off, n)
        src, dst = inputs(peer, me)[kind]
        return pltpu.make_async_remote_copy(
            src_ref=src, dst_ref=dst, send_sem=in_send.at[kind, off], recv_sem=in_recv.at[kind, off],
            device_id={"seq": peer}, device_id_type=MESH,
        )

    def own_copy(kind):
        src, dst = inputs(me, me, True)[kind]
        return pltpu.make_async_copy(src, dst, local_sem.at[kind])

    def input_wait(kind, off):
        peer = flip(me, off, n)
        src, _ = inputs(peer, me)[kind]
        _, dst = inputs(peer, peer)[kind]
        pltpu.make_async_remote_copy(
            src_ref=src, dst_ref=dst, send_sem=in_send.at[kind, off], recv_sem=in_recv.at[kind, off],
            device_id={"seq": peer}, device_id_type=MESH,
        ).wait_recv()

    for kind in range(4):
        own_copy(kind).start()
    for load in loads[:3]:
        load.wait()
    docs = doc_ref[...].astype(jnp.float32)
    for head in range(QUERY_HEADS):
        span = slice(head * hw, (head + 1) * hw)
        prod = do_ref[:, span].astype(jnp.float32) * o_ref[:, span].astype(jnp.float32)
        meta[head // hq, head % hq : head % hq + 1, :] = jnp.sum(prod.T, axis=0, keepdims=True)
    for dest in range(n):
        meta[dest, hq : hq + 1, :] = docs
        if hq + 1 < meta.shape[1]:
            meta[dest, hq + 1 :, :] = jnp.zeros((meta.shape[1] - hq - 1, tokens), jnp.float32)
    loads[3].wait()
    for c in range(x_ref.shape[1] // hw):
        span = slice(c * hw, (c + 1) * hw)
        xt[span, :] = x_ref[:, span].astype(jnp.float32).T.astype(jnp.bfloat16)
    for load in loads[4:]:
        load.wait()
    pl.semaphore_wait(barrier, n - 1 + ndp - 1)

    order = list(range(n - 1, 0, -1))
    for off in order:
        for kind in range(5):
            input_copy(kind, off).start()
    for off in order:
        input_copy(5, off).start()
    own_copy(4).start()
    own_copy(5).start()

    for kind in range(5):
        own_copy(kind).wait()
    for off in order:
        for kind in range(5):
            input_wait(kind, off)

    def dk_slot(source):
        if copies == 1:
            return dk_out.at[:, at(source, hw)]
        return rdk.at[lax.rem(source, copies), :, at(source // copies, hw)]

    def dq_copy(off, arriving=False):
        peer = flip(me, off, n)
        return pltpu.make_async_remote_copy(
            src_ref=dqs.at[peer], dst_ref=dq_out.at[:, at(peer if arriving else me, hq * hw)],
            send_sem=dq_send.at[off], recv_sem=dq_recv.at[off],
            device_id={"seq": peer}, device_id_type=MESH,
        )

    def dk_copy(off, arriving=False):
        peer = flip(me, off, n)
        return pltpu.make_async_remote_copy(
            src_ref=dks.at[peer], dst_ref=dk_slot(peer if arriving else me),
            send_sem=dk_send.at[off], recv_sem=dk_recv.at[off],
            device_id={"seq": peer}, device_id_type=MESH,
        )

    def dq_local():
        return pltpu.make_async_copy(dqs.at[me], dq_out.at[:, at(me, hq * hw)], local_sem.at[6])

    def dk_local():
        return pltpu.make_async_copy(dks.at[me], dk_slot(me), local_sem.at[7])

    def vg_slot(source, i):
        return vg.at[lax.rem(source, copies), at(i, tokens), at(source // copies, hw)]

    def chip_peer(c):
        return partner if c == 0 else flip(chip, c, chips) * CORES + core

    def vg_copy(c, i):
        return pltpu.make_async_remote_copy(
            src_ref=vg_slot(me, i), dst_ref=vg_slot(me, i),
            send_sem=vg_send.at[c, i], recv_sem=vg_recv.at[c, i],
            device_id={"seq": chip_peer(c)}, device_id_type=MESH,
        )

    def vg_wait(c, i):
        pltpu.make_async_remote_copy(
            src_ref=vg_slot(chip_peer(c), i), dst_ref=vg_slot(chip_peer(c), i),
            send_sem=vg_send.at[c, i], recv_sem=vg_recv.at[c, i],
            device_id={"seq": chip_peer(c)}, device_id_type=MESH,
        ).wait_recv()

    direct = [c for c in range(chips) if c < 2 or c % 2 == 0]
    evens = [c for c in direct if c > 1]

    def relay_copy(c, half, i):
        source, target = (1, c - 1) if half == 0 else (c - 1, 1)
        start = i * tokens + half * (tokens // 2)
        origin = chip_peer(source)
        slot = vg.at[lax.rem(origin, copies), at(start // (tokens // 2), tokens // 2), at(origin // copies, hw)]
        return pltpu.make_async_remote_copy(
            src_ref=slot, dst_ref=slot,
            send_sem=relay_send.at[c, half, i], recv_sem=relay_recv.at[c, half, i],
            device_id={"seq": chip_peer(target)}, device_id_type=MESH,
        )

    def relay_wait(c, half, i):
        origin = chip_peer(c)
        start = i * tokens + half * (tokens // 2)
        slot = vg.at[lax.rem(origin, copies), at(start // (tokens // 2), tokens // 2), at(origin // copies, hw)]
        pltpu.make_async_remote_copy(
            src_ref=slot, dst_ref=slot,
            send_sem=relay_send.at[c, half, i], recv_sem=relay_recv.at[c, half, i],
            device_id={"seq": chip_peer(1)}, device_id_type=MESH,
        ).wait_recv()

    def fwd_slot(source):
        return vg.at[lax.rem(source, copies), :, at(source // copies, hw)]

    def fwd_copy(c, source):
        return pltpu.make_async_remote_copy(
            src_ref=fwd_slot(source), dst_ref=fwd_slot(source),
            send_sem=fwd_send.at[c], recv_sem=fwd_recv.at[c],
            device_id={"seq": partner}, device_id_type=MESH,
        )

    for j in range(n):
        dock[at(j, tokens), :] = jnp.broadcast_to(rmeta[j, hq : hq + 1, :], (tokens, tokens)).T

    causal = lax.broadcasted_iota(jnp.int32, (tokens, tokens), 0) <= lax.broadcasted_iota(
        jnp.int32, (tokens, tokens), 1
    )
    for i in reversed(range(n)):
        here = at(i, tokens)
        q2 = jnp.concatenate([rq[here, g * hw : (g + 1) * hw] for g in range(hq)], axis=0)
        do2 = jnp.concatenate([rdo[here, g * hw : (g + 1) * hw] for g in range(hq)], axis=0)
        delta = jnp.concatenate([rmeta[i, g : g + 1, :] for g in range(hq)], axis=1)
        docq = rmeta[i, hq : hq + 1, :]
        window = range(max(0, i - reach), i + 1)
        kept, totals = {}, jnp.zeros((1, hq * tokens), jnp.float32)
        for j in window:
            t = jnp.tanh(nt(rk[at(j, tokens), :], q2) * (query_scale / soft_cap))
            allowed = dock[at(j, tokens), :] == docq
            if i == j:
                allowed = allowed & causal
            mask = jnp.where(allowed, 1.0, 0.0)
            w = jnp.exp(soft_cap * t) * jnp.concatenate([mask] * hq, axis=1)
            totals = totals + jnp.sum(w, axis=0, keepdims=True)
            kept[j] = (t, w)
        inverse = 1.0 / totals
        dq = jnp.zeros((hq * tokens, hw), jnp.float32)
        for j in window:
            t, w = kept[j]
            kj = rk[at(j, tokens), :]
            p = w * inverse
            ds = p * (nt(rv[at(j, tokens), :], do2) - delta) * ((1.0 - t * t) * query_scale)
            ds16, p16 = ds.astype(jnp.bfloat16), p.astype(jnp.bfloat16)
            dk_term = jnp.dot(ds16, q2, preferred_element_type=jnp.float32)
            dv_term = jnp.dot(p16, do2, preferred_element_type=jnp.float32)
            if i == min(n - 1, j + reach):
                dk_acc[at(j, tokens), :] = dk_term
                dv_acc[at(j, tokens), :] = dv_term
            else:
                dk_acc[at(j, tokens), :] += dk_term
                dv_acc[at(j, tokens), :] += dv_term
            dq = dq + tn(ds16, kj)
        vg[lax.rem(me, copies), at(i, tokens), at(me // copies, hw)] = dv_acc[here, :].astype(jnp.bfloat16)
        for g in range(hq):
            dqs[i, :, g * hw : (g + 1) * hw] = dq[g * tokens : (g + 1) * tokens].astype(jnp.bfloat16)
        dks[i] = dk_acc[here, :].astype(jnp.bfloat16)
        for c in reversed(direct):
            vg_copy(c, i).start()

    def out_start(off):
        dq_copy(off).start()
        dk_copy(off).start()

    outgoing = list(range(3, n, 2)) + list(range(2, n, 2)) + [1]
    early = outgoing[:2]
    dq_local().start()
    dk_local().start()

    own_copy(5).wait()
    for off in order:
        input_wait(5, off)

    def z_copy(c, off):
        dest = lax.rem(dme + off, ndp)
        return pltpu.make_async_remote_copy(
            src_ref=zs.at[c, dest], dst_ref=zr.at[c, dme],
            send_sem=z_send.at[c, off], recv_sem=z_recv.at[c, off],
            device_id={"dp": dest}, device_id_type=MESH,
        )

    def z_wait(c, off):
        source = lax.rem(dme + ndp - off, ndp)
        pltpu.make_async_remote_copy(
            src_ref=zs.at[c, source], dst_ref=zr.at[c, source],
            send_sem=z_send.at[c, off], recv_sem=z_recv.at[c, off],
            device_id={"dp": source}, device_id_type=MESH,
        ).wait_recv()

    def weight_term(c):
        columns = at(flip(chip, c, chips), width)
        values = vg[0, :, columns]
        if copies > 1:
            values = values.astype(jnp.float32)
            for other in range(1, copies):
                values = values + vg[other, :, columns].astype(jnp.float32)
            values = values.astype(jnp.bfloat16)
        pf[...] = jnp.dot(rx[...], values, preferred_element_type=jnp.float32)
        for d in range(ndp):
            zs[c, d] = pf[d * piece : (d + 1) * piece, :].astype(jnp.bfloat16)
        for off in range(1, ndp):
            z_copy(c, off).start()

    for i in reversed(range(n)):
        vg_wait(0, i)
    weight_term(0)
    for i in reversed(range(n)):
        if chips > 1:
            vg_wait(1, i)
        for c in evens:
            if c + 1 < chips:
                relay_copy(c + 1, 0, i).start()
        for c in evens:
            vg_wait(c, i)
            if c + 1 < chips:
                relay_copy(c + 1, 1, i).start()
        if i == n // 2:
            for off in early:
                out_start(off)
    for off in outgoing:
        if off not in early:
            out_start(off)
    for c in direct:
        if c:
            fwd_copy(c, chip_peer(c)).start()
    for c in direct:
        if c:
            fwd_copy(c, flip(chip, c, chips) * CORES + (1 - core)).wait_recv()
            weight_term(c)
    for c in range(chips):
        if c not in direct:
            for i in reversed(range(n)):
                relay_wait(c, 0, i)
                relay_wait(c, 1, i)
            fwd_copy(c, chip_peer(c)).start()
            fwd_copy(c, flip(chip, c, chips) * CORES + (1 - core)).wait_recv()
            weight_term(c)

    for c in direct + [c for c in range(chips) if c not in direct]:
        value = zs[c, dme].astype(jnp.float32)
        for off in range(1, ndp):
            z_wait(c, off)
            value = value + zr[c, lax.rem(dme + ndp - off, ndp)].astype(jnp.float32)
        dw_out[:, at(flip(chip, c, chips), width)] = value * total_tokens ** (-0.5)

    for off in order:
        dq_copy(off, True).wait()
        dk_copy(off, True).wait()
    dq_local().wait()
    dk_local().wait()

    if copies > 1:
        total = rdk[0].astype(jnp.float32)
        for other in range(1, copies):
            total = total + rdk[other].astype(jnp.float32)
        dk_out[...] = total.astype(jnp.bfloat16)

    for off in order:
        for kind in range(6):
            input_copy(kind, off).wait_send()
    for c in range(chips):
        for i in range(n):
            if c in direct:
                vg_copy(c, i).wait_send()
            else:
                relay_copy(c, 0, i).wait_send()
                relay_copy(c, 1, i).wait_send()
        if c:
            fwd_copy(c, chip_peer(c)).wait_send()
        for off in range(1, ndp):
            z_copy(c, off).wait_send()


def solution(mesh):
    n, ndp = mesh.shape["seq"], mesh.shape["dp"]

    def local(normed_input, queries, keys, values, saved_output, cotangent, doc_ids):
        tokens = queries.shape[1]
        seq = n * tokens
        hw = HEAD_WIDTH
        hq = QUERY_HEADS // n
        copies = QUERY_HEADS // KEY_VALUE_HEADS // hq
        kvw = keys.shape[2]
        rows = normed_input.shape[2] // n
        piece = rows // ndp
        chips = n // CORES
        width = CORES * hw // copies
        bf, f32 = jnp.bfloat16, jnp.float32
        dma = pltpu.SemaphoreType.DMA
        vmem = pl.BlockSpec(memory_space=pltpu.VMEM)
        dq, dk, dw = pl.pallas_call(
            functools.partial(kernel, n, ndp, float(ndp * seq)),
            out_shape=(
                pltpu.VMEM((tokens, queries.shape[2]), bf),
                pltpu.VMEM((tokens, kvw), bf),
                pltpu.VMEM((piece, kvw), f32),
            ),
            in_specs=[pl.BlockSpec(memory_space=pl.ANY)] * 7,
            out_specs=(vmem, vmem, vmem),
            scratch_shapes=[
                pltpu.VMEM((tokens, normed_input.shape[2]), bf),
                pltpu.VMEM((tokens, queries.shape[2]), bf),
                pltpu.VMEM((tokens, kvw), bf),
                pltpu.VMEM((tokens, kvw), bf),
                pltpu.VMEM((tokens, queries.shape[2]), bf),
                pltpu.VMEM((tokens, queries.shape[2]), bf),
                pltpu.VMEM((1, tokens), jnp.int32),
                pltpu.VMEM((seq, hq * hw), bf),
                pltpu.VMEM((seq, hw), bf),
                pltpu.VMEM((seq, hw), bf),
                pltpu.VMEM((seq, hq * hw), bf),
                pltpu.VMEM((n, 8, tokens), f32),
                pltpu.VMEM((n, 8, tokens), f32),
                pltpu.VMEM((n * rows, tokens), bf),
                pltpu.VMEM((rows, seq), bf),
                pltpu.VMEM((seq, tokens), f32),
                pltpu.VMEM((seq, hw), f32),
                pltpu.VMEM((seq, hw), f32),
                pltpu.VMEM((n, tokens, hq * hw), bf),
                pltpu.VMEM((n, tokens, hw), bf),
                pltpu.VMEM((copies, tokens, kvw), bf),
                pltpu.VMEM((copies, seq, kvw), bf),
                pltpu.VMEM((rows, width), f32),
                pltpu.VMEM((chips, ndp, piece, width), bf),
                pltpu.VMEM((chips, ndp, piece, width), bf),
                dma((7,)), dma((6, n)), dma((6, n)), dma((8,)),
                dma((n,)), dma((n,)), dma((n,)), dma((n,)),
                dma((chips, n)), dma((chips, n)),
                dma((chips, 2, n)), dma((chips, 2, n)), dma((chips,)), dma((chips,)),
                dma((chips, ndp)), dma((chips, ndp)),
            ],
            compiler_params=pltpu.CompilerParams(
                collective_id=0, has_side_effects=True, vmem_limit_bytes=60 * 1024 * 1024
            ),
            name="attention_backward",
        )(normed_input[0], queries[0], keys[0], values[0], saved_output[0], cotangent[0], doc_ids)
        return dq[None], dk[None], dw

    spec = P("dp", "seq", None)
    return jax.shard_map(
        local,
        mesh=mesh,
        in_specs=(spec,) * 6 + (P("dp", "seq"),),
        out_specs=(spec, spec, P(("seq", "dp"), None)),
        check_vma=False,
    )
```

```python
import functools

import jax
import jax.numpy as jnp
from jax import lax
from jax.experimental import pallas as pl
from jax.experimental.pallas import tpu as pltpu
from jax.sharding import PartitionSpec as P

QUERY_HEADS = 16
KEY_VALUE_HEADS = 8
HEAD_WIDTH = 128
CORES = 2
EARLY, MIDDLE = 2, 2
MESH = pl.DeviceIdType.MESH

query_scale = 144.0 ** (-0.5)
soft_cap = 50.0


def flip(index, mask, count):
    out, bit = 0, 1
    while bit < count:
        digit = lax.rem(index // bit, 2)
        out = out + (1 - digit if mask & bit else digit) * bit
        bit *= 2
    return out


def at(index, width):
    start = index * width
    return pl.ds(start if isinstance(index, int) else pl.multiple_of(start, width), width)


def nt(a, b):
    return lax.dot_general(a, b, (((1,), (1,)), ((), ())), preferred_element_type=jnp.float32)


def tn(a, b):
    return lax.dot_general(a, b, (((0,), (0,)), ((), ())), preferred_element_type=jnp.float32)


def kernel(
    n, ndp, total_tokens,
    x_in, q_in, k_in, v_in, o_in, do_in, doc_in,
    dq_out, dk_out, dw_out,
    x_ref, q_ref, k_ref, v_ref, o_ref, do_ref, doc_ref,
    rq, rk, rv, rdo, meta, rmeta, xt, rx, dock,
    dk_acc, dv_acc, dqs, dks, rdk, vg, pf, zs, zr,
    load_sem, in_send, in_recv, local_sem, out_send, out_recv, vg_send, near_recv, vg_recv,
    relay_recv, fwd_recv, z_recv, seq_sem, dp_sem,
):
    me = lax.axis_index("seq")
    dme = lax.axis_index("dp")
    tokens = q_ref.shape[0]
    seq = n * tokens
    hw = HEAD_WIDTH
    group = QUERY_HEADS // KEY_VALUE_HEADS
    hq = QUERY_HEADS // n
    copies = group // hq
    rows = x_ref.shape[1] // n
    piece = rows // ndp
    chips = n // CORES
    width = CORES * hw // copies
    reach = (seq // 2 - 1 + tokens - 1) // tokens
    chip, core = me // CORES, lax.rem(me, CORES)
    partner = chip * CORES + (1 - core)

    bits = [1 << b for b in range(n.bit_length() - 1)]
    below, above = dme > 0, dme < ndp - 1
    barrier = pltpu.get_barrier_semaphore()
    for bit in reversed(bits):
        pl.semaphore_signal(barrier, inc=1, device_id={"seq": flip(me, bit, n)}, device_id_type=MESH)

    def tell_dp(up, down):
        @pl.when(above)
        def _():
            pl.semaphore_signal(up, inc=1, device_id={"dp": dme + 1}, device_id_type=MESH)

        @pl.when(below)
        def _():
            pl.semaphore_signal(down, inc=1, device_id={"dp": dme - 1}, device_id_type=MESH)

    tell_dp(barrier, barrier)

    loads = [
        pltpu.make_async_copy(src, dst, load_sem.at[index])
        for index, (src, dst) in enumerate((
            (do_in, do_ref), (o_in, o_ref), (doc_in, doc_ref), (x_in, x_ref),
            (k_in, k_ref), (v_in, v_ref), (q_in, q_ref),
        ))
    ]
    for load in loads:
        load.start()

    def inputs(dest, slot, local=False):
        kv = dest * hq // group
        sources = (k_in, v_in, q_in, do_in) if local else (k_ref, v_ref, q_ref, do_ref)
        return [
            (sources[0].at[:, at(kv, hw)], rk.at[at(slot, tokens), :]),
            (sources[1].at[:, at(kv, hw)], rv.at[at(slot, tokens), :]),
            (sources[2].at[:, at(dest, hq * hw)], rq.at[at(slot, tokens), :]),
            (sources[3].at[:, at(dest, hq * hw)], rdo.at[at(slot, tokens), :]),
            (meta.at[dest], rmeta.at[slot]),
            (xt.at[at(dest, rows), :], rx.at[:, at(slot, tokens)]),
        ]

    def input_copy(kind, off):
        peer = flip(me, off, n)
        src, dst = inputs(peer, me)[kind]
        return pltpu.make_async_remote_copy(
            src_ref=src, dst_ref=dst, send_sem=in_send.at[kind], recv_sem=in_recv.at[kind],
            device_id={"seq": peer}, device_id_type=MESH,
        )

    def own_copy(kind):
        src, dst = inputs(me, me, True)[kind]
        return pltpu.make_async_copy(src, dst, local_sem.at[kind])

    def bulk(ref, sem):
        return pltpu.make_async_remote_copy(
            src_ref=ref, dst_ref=ref, send_sem=sem, recv_sem=sem,
            device_id={"seq": partner}, device_id_type=MESH,
        )

    rest = pl.ds(0, (n - 1) * tokens)
    others = [
        rk.at[rest, :], rv.at[rest, :], rq.at[rest, :], rdo.at[rest, :], rmeta.at[pl.ds(0, n - 1)],
        xt.at[pl.ds(0, (n - 1) * rows), :],
    ]

    for kind in range(4):
        own_copy(kind).start()
    for load in loads[:3]:
        load.wait()
    docs = doc_ref[...].astype(jnp.float32)
    for head in range(QUERY_HEADS):
        span = slice(head * hw, (head + 1) * hw)
        prod = do_ref[:, span].astype(jnp.float32) * o_ref[:, span].astype(jnp.float32)
        meta[head // hq, head % hq : head % hq + 1, :] = jnp.sum(prod.T, axis=0, keepdims=True)
    for dest in range(n):
        meta[dest, hq : hq + 1, :] = docs
        if hq + 1 < meta.shape[1]:
            meta[dest, hq + 1 :, :] = jnp.zeros((meta.shape[1] - hq - 1, tokens), jnp.float32)
    loads[3].wait()
    for c in range(x_ref.shape[1] // hw):
        span = slice(c * hw, (c + 1) * hw)
        xt[span, :] = x_ref[:, span].astype(jnp.float32).T.astype(jnp.bfloat16)
    for load in loads[4:]:
        load.wait()
    pl.semaphore_wait(barrier, len(bits) + below.astype(jnp.int32) + above.astype(jnp.int32))

    for distance in range(1, len(bits) + 1):
        if distance > 1:
            for b, bit in enumerate(bits):
                pl.semaphore_signal(
                    seq_sem.at[distance - 2, b], inc=1, device_id={"seq": flip(me, bit, n)}, device_id_type=MESH
                )
            for b in range(len(bits)):
                pl.semaphore_wait(seq_sem.at[distance - 2, b], 1)
        for off in range(n - 1, 0, -1):
            if off.bit_count() == distance:
                for kind in range(5):
                    input_copy(kind, off).start()
    for off in range(n - 1, 0, -1):
        input_copy(5, off).start()
    own_copy(4).start()
    own_copy(5).start()

    for step in range(ndp - 2):
        tell_dp(dp_sem.at[step, 0], dp_sem.at[step, 1])

        @pl.when(below)
        def _():
            pl.semaphore_wait(dp_sem.at[step, 0], 1)

        @pl.when(above)
        def _():
            pl.semaphore_wait(dp_sem.at[step, 1], 1)

    for kind in range(5):
        own_copy(kind).wait()
    for kind in range(5):
        bulk(others[kind], in_recv.at[kind]).wait_recv()

    def dk_slot(source):
        if copies == 1:
            return dk_out.at[:, at(source, hw)]
        return rdk.at[lax.rem(source, copies), :, at(source // copies, hw)]

    def dq_copy(off):
        peer = flip(me, off, n)
        return pltpu.make_async_remote_copy(
            src_ref=dqs.at[peer], dst_ref=dq_out.at[:, at(me, hq * hw)],
            send_sem=out_send.at[0], recv_sem=out_recv.at[0],
            device_id={"seq": peer}, device_id_type=MESH,
        )

    def dk_copy(off):
        peer = flip(me, off, n)
        return pltpu.make_async_remote_copy(
            src_ref=dks.at[peer], dst_ref=dk_slot(me),
            send_sem=out_send.at[1], recv_sem=out_recv.at[1],
            device_id={"seq": peer}, device_id_type=MESH,
        )

    def dq_local():
        return pltpu.make_async_copy(dqs.at[me], dq_out.at[:, at(me, hq * hw)], local_sem.at[6])

    def dk_local():
        return pltpu.make_async_copy(dks.at[me], dk_slot(me), local_sem.at[7])

    def vg_slot(source, i):
        return vg.at[lax.rem(source, copies), at(i, tokens), at(source // copies, hw)]

    def chip_peer(c):
        return partner if c == 0 else flip(chip, c, chips) * CORES + core

    def vg_arrival(c, i):
        return near_recv.at[0] if c == 0 else vg_recv.at[c // 2, i]

    def vg_copy(c, i):
        return pltpu.make_async_remote_copy(
            src_ref=vg_slot(me, i), dst_ref=vg_slot(me, i),
            send_sem=vg_send.at[0], recv_sem=vg_arrival(c, i),
            device_id={"seq": chip_peer(c)}, device_id_type=MESH,
        )

    direct = [c for c in range(chips) if c < 2 or c % 2 == 0]
    evens = [c for c in direct if c > 1]

    def relay_copy(c, half, i):
        source, target = (1, c - 1) if half == 0 else (c - 1, 1)
        start = i * tokens + half * (tokens // 2)
        origin = chip_peer(source)
        slot = vg.at[lax.rem(origin, copies), at(start // (tokens // 2), tokens // 2), at(origin // copies, hw)]
        return pltpu.make_async_remote_copy(
            src_ref=slot, dst_ref=slot,
            send_sem=vg_send.at[1], recv_sem=relay_recv.at[c // 2],
            device_id={"seq": chip_peer(target)}, device_id_type=MESH,
        )

    def fwd_slot(source):
        return vg.at[lax.rem(source, copies), :, at(source // copies, hw)]

    def fwd_copy(c, source):
        return pltpu.make_async_remote_copy(
            src_ref=fwd_slot(source), dst_ref=fwd_slot(source),
            send_sem=vg_send.at[2], recv_sem=fwd_recv.at[c],
            device_id={"seq": partner}, device_id_type=MESH,
        )

    for j in range(n):
        dock[at(j, tokens), :] = jnp.broadcast_to(rmeta[j, hq : hq + 1, :], (tokens, tokens)).T

    causal = lax.broadcasted_iota(jnp.int32, (tokens, tokens), 0) <= lax.broadcasted_iota(
        jnp.int32, (tokens, tokens), 1
    )
    for i in reversed(range(n)):
        here = at(i, tokens)
        q2 = jnp.concatenate([rq[here, g * hw : (g + 1) * hw] for g in range(hq)], axis=0)
        do2 = jnp.concatenate([rdo[here, g * hw : (g + 1) * hw] for g in range(hq)], axis=0)
        delta = jnp.concatenate([rmeta[i, g : g + 1, :] for g in range(hq)], axis=1)
        docq = rmeta[i, hq : hq + 1, :]
        window = range(max(0, i - reach), i + 1)
        kept, totals = {}, jnp.zeros((1, hq * tokens), jnp.float32)
        for j in window:
            t = jnp.tanh(nt(rk[at(j, tokens), :], q2) * (query_scale / soft_cap))
            allowed = dock[at(j, tokens), :] == docq
            if i == j:
                allowed = allowed & causal
            mask = jnp.where(allowed, 1.0, 0.0)
            w = jnp.exp(soft_cap * t) * jnp.concatenate([mask] * hq, axis=1)
            totals = totals + jnp.sum(w, axis=0, keepdims=True)
            kept[j] = (t, w)
        inverse = 1.0 / totals
        dq = jnp.zeros((hq * tokens, hw), jnp.float32)
        for j in window:
            t, w = kept[j]
            kj = rk[at(j, tokens), :]
            p = w * inverse
            ds = p * (nt(rv[at(j, tokens), :], do2) - delta) * ((1.0 - t * t) * query_scale)
            ds16, p16 = ds.astype(jnp.bfloat16), p.astype(jnp.bfloat16)
            dk_term = jnp.dot(ds16, q2, preferred_element_type=jnp.float32)
            dv_term = jnp.dot(p16, do2, preferred_element_type=jnp.float32)
            if i == min(n - 1, j + reach):
                dk_acc[at(j, tokens), :] = dk_term
                dv_acc[at(j, tokens), :] = dv_term
            else:
                dk_acc[at(j, tokens), :] += dk_term
                dv_acc[at(j, tokens), :] += dv_term
            dq = dq + tn(ds16, kj)
        vg[lax.rem(me, copies), at(i, tokens), at(me // copies, hw)] = dv_acc[here, :].astype(jnp.bfloat16)
        for g in range(hq):
            dqs[i, :, g * hw : (g + 1) * hw] = dq[g * tokens : (g + 1) * tokens].astype(jnp.bfloat16)
        dks[i] = dk_acc[here, :].astype(jnp.bfloat16)
        for c in reversed(direct):
            vg_copy(c, i).start()

    def out_start(off):
        dq_copy(off).start()
        dk_copy(off).start()

    outgoing = list(range(3, n, 2)) + list(range(2, n, 2)) + [1]
    dq_local().start()
    dk_local().start()

    own_copy(5).wait()
    bulk(others[5], in_recv.at[5]).wait_recv()

    def z_copy(c, off):
        dest = lax.rem(dme + off, ndp)
        return pltpu.make_async_remote_copy(
            src_ref=zs.at[c, dest], dst_ref=zr.at[c, dme],
            send_sem=vg_send.at[3], recv_sem=z_recv.at[c],
            device_id={"dp": dest}, device_id_type=MESH,
        )

    def weight_term(c):
        columns = at(flip(chip, c, chips), width)
        values = vg[0, :, columns]
        if copies > 1:
            values = values.astype(jnp.float32)
            for other in range(1, copies):
                values = values + vg[other, :, columns].astype(jnp.float32)
            values = values.astype(jnp.bfloat16)
        pf[...] = jnp.dot(rx[...], values, preferred_element_type=jnp.float32)
        for d in range(ndp):
            zs[c, d] = pf[d * piece : (d + 1) * piece, :].astype(jnp.bfloat16)
        for off in range(1, ndp):
            z_copy(c, off).start()

    bulk(fwd_slot(partner), near_recv.at[0]).wait_recv()
    weight_term(0)
    for i in reversed(range(n)):
        if chips > 1:
            bulk(vg_slot(chip_peer(1), i), vg_arrival(1, i)).wait_recv()
        for c in evens:
            if c + 1 < chips:
                relay_copy(c + 1, 0, i).start()
        for c in evens:
            bulk(vg_slot(chip_peer(c), i), vg_arrival(c, i)).wait_recv()
            if c + 1 < chips:
                relay_copy(c + 1, 1, i).start()
        if i == n // 2:
            for off in outgoing[:EARLY]:
                out_start(off)
    for c in direct:
        if c:
            fwd_copy(c, chip_peer(c)).start()
    for off in outgoing[EARLY:MIDDLE]:
        out_start(off)
    for c in direct:
        if c:
            bulk(fwd_slot(flip(chip, c, chips) * CORES + (1 - core)), fwd_recv.at[c]).wait_recv()
            weight_term(c)
    relayed = [c for c in range(chips) if c not in direct]
    for c in relayed:
        bulk(fwd_slot(chip_peer(c)), relay_recv.at[c // 2]).wait_recv()
        fwd_copy(c, chip_peer(c)).start()
    for off in outgoing[MIDDLE:]:
        out_start(off)
    for c in relayed:
        bulk(fwd_slot(flip(chip, c, chips) * CORES + (1 - core)), fwd_recv.at[c]).wait_recv()
        weight_term(c)

    for c in direct + relayed:
        value = zs[c, dme].astype(jnp.float32)
        bulk(zr.at[c, pl.ds(0, ndp - 1)], z_recv.at[c]).wait_recv()
        for off in range(1, ndp):
            value = value + zr[c, lax.rem(dme + ndp - off, ndp)].astype(jnp.float32)
        dw_out[:, at(flip(chip, c, chips), width)] = value * total_tokens ** (-0.5)

    for index, ref in enumerate((dqs, dks)):
        bulk(ref.at[pl.ds(0, n - 1)], out_recv.at[index]).wait_recv()
    dq_local().wait()
    dk_local().wait()

    if copies > 1:
        total = rdk[0].astype(jnp.float32)
        for other in range(1, copies):
            total = total + rdk[other].astype(jnp.float32)
        dk_out[...] = total.astype(jnp.bfloat16)

    for kind in range(6):
        bulk(others[kind], in_send.at[kind]).wait_send()
    for index, ref in enumerate((dqs, dks)):
        bulk(ref.at[pl.ds(0, n - 1)], out_send.at[index]).wait_send()
    for index, count in enumerate((len(direct), len(relayed), chips - 1)):
        if count:
            bulk(vg.at[0, :, pl.ds(0, count * hw)], vg_send.at[index]).wait_send()
    bulk(zs.at[:, pl.ds(0, ndp - 1)], vg_send.at[3]).wait_send()


def solution(mesh):
    n, ndp = mesh.shape["seq"], mesh.shape["dp"]

    def local(normed_input, queries, keys, values, saved_output, cotangent, doc_ids):
        tokens = queries.shape[1]
        seq = n * tokens
        hw = HEAD_WIDTH
        hq = QUERY_HEADS // n
        copies = QUERY_HEADS // KEY_VALUE_HEADS // hq
        kvw = keys.shape[2]
        rows = normed_input.shape[2] // n
        piece = rows // ndp
        chips = n // CORES
        width = CORES * hw // copies
        bf, f32 = jnp.bfloat16, jnp.float32
        dma = pltpu.SemaphoreType.DMA
        vmem = pl.BlockSpec(memory_space=pltpu.VMEM)
        dq, dk, dw = pl.pallas_call(
            functools.partial(kernel, n, ndp, float(ndp * seq)),
            out_shape=(
                pltpu.VMEM((tokens, queries.shape[2]), bf),
                pltpu.VMEM((tokens, kvw), bf),
                pltpu.VMEM((piece, kvw), f32),
            ),
            in_specs=[pl.BlockSpec(memory_space=pl.ANY)] * 7,
            out_specs=(vmem, vmem, vmem),
            scratch_shapes=[
                pltpu.VMEM((tokens, normed_input.shape[2]), bf),
                pltpu.VMEM((tokens, queries.shape[2]), bf),
                pltpu.VMEM((tokens, kvw), bf),
                pltpu.VMEM((tokens, kvw), bf),
                pltpu.VMEM((tokens, queries.shape[2]), bf),
                pltpu.VMEM((tokens, queries.shape[2]), bf),
                pltpu.VMEM((1, tokens), jnp.int32),
                pltpu.VMEM((seq, hq * hw), bf),
                pltpu.VMEM((seq, hw), bf),
                pltpu.VMEM((seq, hw), bf),
                pltpu.VMEM((seq, hq * hw), bf),
                pltpu.VMEM((n, 8, tokens), f32),
                pltpu.VMEM((n, 8, tokens), f32),
                pltpu.VMEM((n * rows, tokens), bf),
                pltpu.VMEM((rows, seq), bf),
                pltpu.VMEM((seq, tokens), f32),
                pltpu.VMEM((seq, hw), f32),
                pltpu.VMEM((seq, hw), f32),
                pltpu.VMEM((n, tokens, hq * hw), bf),
                pltpu.VMEM((n, tokens, hw), bf),
                pltpu.VMEM((copies, tokens, kvw), bf),
                pltpu.VMEM((copies, seq, kvw), bf),
                pltpu.VMEM((rows, width), f32),
                pltpu.VMEM((chips, ndp, piece, width), bf),
                pltpu.VMEM((chips, ndp, piece, width), bf),
                dma((7,)), dma((6,)), dma((6,)), dma((8,)), dma((2,)), dma((2,)),
                dma((4,)), dma((1,)), dma((chips // 2, n)), dma((chips // 2,)), dma((chips,)), dma((chips,)),
                pltpu.SemaphoreType.REGULAR((max(1, n.bit_length() - 2), n.bit_length() - 1)),
                pltpu.SemaphoreType.REGULAR((max(1, ndp - 2), 2)),
            ],
            compiler_params=pltpu.CompilerParams(
                collective_id=0, has_side_effects=True, vmem_limit_bytes=60 * 1024 * 1024
            ),
            name="attention_backward",
        )(normed_input[0], queries[0], keys[0], values[0], saved_output[0], cotangent[0], doc_ids)
        return dq[None], dk[None], dw

    spec = P("dp", "seq", None)
    return jax.shard_map(
        local,
        mesh=mesh,
        in_specs=(spec,) * 6 + (P("dp", "seq"),),
        out_specs=(spec, spec, P(("seq", "dp"), None)),
        check_vma=False,
    )
```

```python
import functools

import jax
import jax.numpy as jnp
from jax import lax
from jax.experimental import pallas as pl
from jax.experimental.pallas import tpu as pltpu
from jax.sharding import PartitionSpec as P

QUERY_HEADS = 16
KEY_VALUE_HEADS = 8
HEAD_WIDTH = 128
CORES = 2
EARLY, MIDDLE = 2, 4
MESH = pl.DeviceIdType.MESH

query_scale = 144.0 ** (-0.5)
soft_cap = 50.0


def flip(index, mask, count):
    out, bit = 0, 1
    while bit < count:
        digit = lax.rem(index // bit, 2)
        out = out + (1 - digit if mask & bit else digit) * bit
        bit *= 2
    return out


def at(index, width):
    start = index * width
    return pl.ds(start if isinstance(index, int) else pl.multiple_of(start, width), width)


def nt(a, b):
    return lax.dot_general(a, b, (((1,), (1,)), ((), ())), preferred_element_type=jnp.float32)


def tn(a, b):
    return lax.dot_general(a, b, (((0,), (0,)), ((), ())), preferred_element_type=jnp.float32)


def kernel(
    n, ndp, total_tokens,
    x_in, q_in, k_in, v_in, o_in, do_in, doc_in,
    dq_out, dk_out, dw_out,
    x_ref, q_ref, k_ref, v_ref, o_ref, do_ref, doc_ref,
    rq, rk, rv, rdo, meta, rmeta, xt, rx, dock,
    dk_acc, dv_acc, dqs, dks, rdk, vg, pf, zs, zr,
    load_sem, in_send, in_recv, local_sem, out_send, out_recv, vg_send, near_recv, vg_recv,
    relay_recv, fwd_recv, z_recv, dp_sem,
):
    me = lax.axis_index("seq")
    dme = lax.axis_index("dp")
    tokens = q_ref.shape[0]
    seq = n * tokens
    hw = HEAD_WIDTH
    group = QUERY_HEADS // KEY_VALUE_HEADS
    hq = QUERY_HEADS // n
    copies = group // hq
    rows = x_ref.shape[1] // n
    piece = rows // ndp
    chips = n // CORES
    width = CORES * hw // copies
    reach = (seq // 2 - 1 + tokens - 1) // tokens
    chip, core = me // CORES, lax.rem(me, CORES)
    partner = chip * CORES + (1 - core)

    below, above = dme > 0, dme < ndp - 1
    barrier = pltpu.get_barrier_semaphore()
    for off in range(n - 1, 0, -1):
        pl.semaphore_signal(barrier, inc=1, device_id={"seq": flip(me, off, n)}, device_id_type=MESH)

    def tell_dp(up, down):
        @pl.when(above)
        def _():
            pl.semaphore_signal(up, inc=1, device_id={"dp": dme + 1}, device_id_type=MESH)

        @pl.when(below)
        def _():
            pl.semaphore_signal(down, inc=1, device_id={"dp": dme - 1}, device_id_type=MESH)

    tell_dp(barrier, barrier)

    loads = [
        pltpu.make_async_copy(src, dst, load_sem.at[index])
        for index, (src, dst) in enumerate((
            (do_in, do_ref), (o_in, o_ref), (doc_in, doc_ref), (x_in, x_ref),
            (k_in, k_ref), (v_in, v_ref), (q_in, q_ref),
        ))
    ]
    for load in loads:
        load.start()

    def inputs(dest, slot, local=False):
        kv = dest * hq // group
        sources = (k_in, v_in, q_in, do_in) if local else (k_ref, v_ref, q_ref, do_ref)
        return [
            (sources[0].at[:, at(kv, hw)], rk.at[at(slot, tokens), :]),
            (sources[1].at[:, at(kv, hw)], rv.at[at(slot, tokens), :]),
            (sources[2].at[:, at(dest, hq * hw)], rq.at[at(slot, tokens), :]),
            (sources[3].at[:, at(dest, hq * hw)], rdo.at[at(slot, tokens), :]),
            (meta.at[dest], rmeta.at[slot]),
            (xt.at[at(dest, rows), :], rx.at[:, at(slot, tokens)]),
        ]

    def input_copy(kind, off):
        peer = flip(me, off, n)
        src, dst = inputs(peer, me)[kind]
        return pltpu.make_async_remote_copy(
            src_ref=src, dst_ref=dst, send_sem=in_send.at[kind], recv_sem=in_recv.at[kind],
            device_id={"seq": peer}, device_id_type=MESH,
        )

    def own_copy(kind):
        src, dst = inputs(me, me, True)[kind]
        return pltpu.make_async_copy(src, dst, local_sem.at[kind])

    def bulk(ref, sem):
        return pltpu.make_async_remote_copy(
            src_ref=ref, dst_ref=ref, send_sem=sem, recv_sem=sem,
            device_id={"seq": partner}, device_id_type=MESH,
        )

    rest = pl.ds(0, (n - 1) * tokens)
    others = [
        rk.at[rest, :], rv.at[rest, :], rq.at[rest, :], rdo.at[rest, :], rmeta.at[pl.ds(0, n - 1)],
        xt.at[pl.ds(0, (n - 1) * rows), :],
    ]

    for kind in range(4):
        own_copy(kind).start()
    for load in loads[:3]:
        load.wait()
    docs = doc_ref[...].astype(jnp.float32)
    for head in range(QUERY_HEADS):
        span = slice(head * hw, (head + 1) * hw)
        prod = do_ref[:, span].astype(jnp.float32) * o_ref[:, span].astype(jnp.float32)
        meta[head // hq, head % hq : head % hq + 1, :] = jnp.sum(prod.T, axis=0, keepdims=True)
    for dest in range(n):
        meta[dest, hq : hq + 1, :] = docs
        if hq + 1 < meta.shape[1]:
            meta[dest, hq + 1 :, :] = jnp.zeros((meta.shape[1] - hq - 1, tokens), jnp.float32)
    loads[3].wait()
    for c in range(x_ref.shape[1] // hw):
        span = slice(c * hw, (c + 1) * hw)
        xt[span, :] = x_ref[:, span].astype(jnp.float32).T.astype(jnp.bfloat16)
    for load in loads[4:]:
        load.wait()
    pl.semaphore_wait(barrier, n - 1 + below.astype(jnp.int32) + above.astype(jnp.int32))

    order = list(range(n - 1, 0, -1))
    for off in order:
        for kind in range(5):
            input_copy(kind, off).start()
    for off in order:
        input_copy(5, off).start()
    own_copy(4).start()
    own_copy(5).start()

    for step in range(ndp - 2):
        tell_dp(dp_sem.at[step, 0], dp_sem.at[step, 1])

        @pl.when(below)
        def _():
            pl.semaphore_wait(dp_sem.at[step, 0], 1)

        @pl.when(above)
        def _():
            pl.semaphore_wait(dp_sem.at[step, 1], 1)

    for kind in range(5):
        own_copy(kind).wait()
    for kind in range(5):
        bulk(others[kind], in_recv.at[kind]).wait_recv()

    def dk_slot(source):
        if copies == 1:
            return dk_out.at[:, at(source, hw)]
        return rdk.at[lax.rem(source, copies), :, at(source // copies, hw)]

    def dq_copy(off):
        peer = flip(me, off, n)
        return pltpu.make_async_remote_copy(
            src_ref=dqs.at[peer], dst_ref=dq_out.at[:, at(me, hq * hw)],
            send_sem=out_send.at[0], recv_sem=out_recv.at[0],
            device_id={"seq": peer}, device_id_type=MESH,
        )

    def dk_copy(off):
        peer = flip(me, off, n)
        return pltpu.make_async_remote_copy(
            src_ref=dks.at[peer], dst_ref=dk_slot(me),
            send_sem=out_send.at[1], recv_sem=out_recv.at[1],
            device_id={"seq": peer}, device_id_type=MESH,
        )

    def dq_local():
        return pltpu.make_async_copy(dqs.at[me], dq_out.at[:, at(me, hq * hw)], local_sem.at[6])

    def dk_local():
        return pltpu.make_async_copy(dks.at[me], dk_slot(me), local_sem.at[7])

    def vg_slot(source, i):
        return vg.at[lax.rem(source, copies), at(i, tokens), at(source // copies, hw)]

    def chip_peer(c):
        return partner if c == 0 else flip(chip, c, chips) * CORES + core

    def vg_arrival(c, i):
        return near_recv.at[0] if c == 0 else vg_recv.at[c // 2, i]

    def vg_copy(c, i):
        return pltpu.make_async_remote_copy(
            src_ref=vg_slot(me, i), dst_ref=vg_slot(me, i),
            send_sem=vg_send.at[0], recv_sem=vg_arrival(c, i),
            device_id={"seq": chip_peer(c)}, device_id_type=MESH,
        )

    direct = [c for c in range(chips) if c < 2 or c % 2 == 0]
    evens = [c for c in direct if c > 1]

    def relay_copy(c, half, i):
        source, target = (1, c - 1) if half == 0 else (c - 1, 1)
        start = i * tokens + half * (tokens // 2)
        origin = chip_peer(source)
        slot = vg.at[lax.rem(origin, copies), at(start // (tokens // 2), tokens // 2), at(origin // copies, hw)]
        return pltpu.make_async_remote_copy(
            src_ref=slot, dst_ref=slot,
            send_sem=vg_send.at[1], recv_sem=relay_recv.at[c // 2],
            device_id={"seq": chip_peer(target)}, device_id_type=MESH,
        )

    def fwd_slot(source):
        return vg.at[lax.rem(source, copies), :, at(source // copies, hw)]

    def fwd_copy(c, source):
        return pltpu.make_async_remote_copy(
            src_ref=fwd_slot(source), dst_ref=fwd_slot(source),
            send_sem=vg_send.at[2], recv_sem=fwd_recv.at[c],
            device_id={"seq": partner}, device_id_type=MESH,
        )

    for j in range(n):
        dock[at(j, tokens), :] = jnp.broadcast_to(rmeta[j, hq : hq + 1, :], (tokens, tokens)).T

    causal = lax.broadcasted_iota(jnp.int32, (tokens, tokens), 0) <= lax.broadcasted_iota(
        jnp.int32, (tokens, tokens), 1
    )
    for i in reversed(range(n)):
        here = at(i, tokens)
        q2 = jnp.concatenate([rq[here, g * hw : (g + 1) * hw] for g in range(hq)], axis=0)
        do2 = jnp.concatenate([rdo[here, g * hw : (g + 1) * hw] for g in range(hq)], axis=0)
        delta = jnp.concatenate([rmeta[i, g : g + 1, :] for g in range(hq)], axis=1)
        docq = rmeta[i, hq : hq + 1, :]
        window = range(max(0, i - reach), i + 1)
        kept, totals = {}, jnp.zeros((1, hq * tokens), jnp.float32)
        for j in window:
            t = jnp.tanh(nt(rk[at(j, tokens), :], q2) * (query_scale / soft_cap))
            allowed = dock[at(j, tokens), :] == docq
            if i == j:
                allowed = allowed & causal
            mask = jnp.where(allowed, 1.0, 0.0)
            w = jnp.exp(soft_cap * t) * jnp.concatenate([mask] * hq, axis=1)
            totals = totals + jnp.sum(w, axis=0, keepdims=True)
            kept[j] = (t, w)
        inverse = 1.0 / totals
        dq = jnp.zeros((hq * tokens, hw), jnp.float32)
        for j in window:
            t, w = kept[j]
            kj = rk[at(j, tokens), :]
            p = w * inverse
            ds = p * (nt(rv[at(j, tokens), :], do2) - delta) * ((1.0 - t * t) * query_scale)
            ds16, p16 = ds.astype(jnp.bfloat16), p.astype(jnp.bfloat16)
            dk_term = jnp.dot(ds16, q2, preferred_element_type=jnp.float32)
            dv_term = jnp.dot(p16, do2, preferred_element_type=jnp.float32)
            if i == min(n - 1, j + reach):
                dk_acc[at(j, tokens), :] = dk_term
                dv_acc[at(j, tokens), :] = dv_term
            else:
                dk_acc[at(j, tokens), :] += dk_term
                dv_acc[at(j, tokens), :] += dv_term
            dq = dq + tn(ds16, kj)
        vg[lax.rem(me, copies), at(i, tokens), at(me // copies, hw)] = dv_acc[here, :].astype(jnp.bfloat16)
        for g in range(hq):
            dqs[i, :, g * hw : (g + 1) * hw] = dq[g * tokens : (g + 1) * tokens].astype(jnp.bfloat16)
        dks[i] = dk_acc[here, :].astype(jnp.bfloat16)
        for c in reversed(direct):
            vg_copy(c, i).start()

    def out_start(off):
        dq_copy(off).start()
        dk_copy(off).start()

    outgoing = list(range(3, n, 2)) + list(range(2, n, 2)) + [1]
    dq_local().start()
    dk_local().start()

    own_copy(5).wait()
    bulk(others[5], in_recv.at[5]).wait_recv()

    def z_copy(c, off):
        dest = lax.rem(dme + off, ndp)
        return pltpu.make_async_remote_copy(
            src_ref=zs.at[c, dest], dst_ref=zr.at[c, dme],
            send_sem=vg_send.at[3], recv_sem=z_recv.at[c],
            device_id={"dp": dest}, device_id_type=MESH,
        )

    def weight_term(c):
        columns = at(flip(chip, c, chips), width)
        values = vg[0, :, columns]
        if copies > 1:
            values = values.astype(jnp.float32)
            for other in range(1, copies):
                values = values + vg[other, :, columns].astype(jnp.float32)
            values = values.astype(jnp.bfloat16)
        pf[...] = jnp.dot(rx[...], values, preferred_element_type=jnp.float32)
        for d in range(ndp):
            zs[c, d] = pf[d * piece : (d + 1) * piece, :].astype(jnp.bfloat16)
        for off in range(1, ndp):
            z_copy(c, off).start()

    bulk(fwd_slot(partner), near_recv.at[0]).wait_recv()
    weight_term(0)
    for i in reversed(range(n)):
        if chips > 1:
            bulk(vg_slot(chip_peer(1), i), vg_arrival(1, i)).wait_recv()
        for c in evens:
            if c + 1 < chips:
                relay_copy(c + 1, 0, i).start()
        for c in evens:
            bulk(vg_slot(chip_peer(c), i), vg_arrival(c, i)).wait_recv()
            if c + 1 < chips:
                relay_copy(c + 1, 1, i).start()
        if i == n // 2:
            for off in outgoing[:EARLY]:
                out_start(off)
    for c in direct:
        if c:
            fwd_copy(c, chip_peer(c)).start()
    for off in outgoing[EARLY:MIDDLE]:
        out_start(off)
    for c in direct:
        if c:
            bulk(fwd_slot(flip(chip, c, chips) * CORES + (1 - core)), fwd_recv.at[c]).wait_recv()
            weight_term(c)
    relayed = [c for c in range(chips) if c not in direct]
    for c in relayed:
        bulk(fwd_slot(chip_peer(c)), relay_recv.at[c // 2]).wait_recv()
        fwd_copy(c, chip_peer(c)).start()
    for off in outgoing[MIDDLE:]:
        out_start(off)
    for c in relayed:
        bulk(fwd_slot(flip(chip, c, chips) * CORES + (1 - core)), fwd_recv.at[c]).wait_recv()
        weight_term(c)

    for c in direct + relayed:
        value = zs[c, dme].astype(jnp.float32)
        bulk(zr.at[c, pl.ds(0, ndp - 1)], z_recv.at[c]).wait_recv()
        for off in range(1, ndp):
            value = value + zr[c, lax.rem(dme + ndp - off, ndp)].astype(jnp.float32)
        dw_out[:, at(flip(chip, c, chips), width)] = value * total_tokens ** (-0.5)

    for index, ref in enumerate((dqs, dks)):
        bulk(ref.at[pl.ds(0, n - 1)], out_recv.at[index]).wait_recv()
    dq_local().wait()
    dk_local().wait()

    if copies > 1:
        total = rdk[0].astype(jnp.float32)
        for other in range(1, copies):
            total = total + rdk[other].astype(jnp.float32)
        dk_out[...] = total.astype(jnp.bfloat16)

    for kind in range(6):
        bulk(others[kind], in_send.at[kind]).wait_send()
    for index, ref in enumerate((dqs, dks)):
        bulk(ref.at[pl.ds(0, n - 1)], out_send.at[index]).wait_send()
    for index, count in enumerate((len(direct), len(relayed), chips - 1)):
        if count:
            bulk(vg.at[0, :, pl.ds(0, count * hw)], vg_send.at[index]).wait_send()
    bulk(zs.at[:, pl.ds(0, ndp - 1)], vg_send.at[3]).wait_send()


def solution(mesh):
    n, ndp = mesh.shape["seq"], mesh.shape["dp"]

    def local(normed_input, queries, keys, values, saved_output, cotangent, doc_ids):
        tokens = queries.shape[1]
        seq = n * tokens
        hw = HEAD_WIDTH
        hq = QUERY_HEADS // n
        copies = QUERY_HEADS // KEY_VALUE_HEADS // hq
        kvw = keys.shape[2]
        rows = normed_input.shape[2] // n
        piece = rows // ndp
        chips = n // CORES
        width = CORES * hw // copies
        bf, f32 = jnp.bfloat16, jnp.float32
        dma = pltpu.SemaphoreType.DMA
        vmem = pl.BlockSpec(memory_space=pltpu.VMEM)
        dq, dk, dw = pl.pallas_call(
            functools.partial(kernel, n, ndp, float(ndp * seq)),
            out_shape=(
                pltpu.VMEM((tokens, queries.shape[2]), bf),
                pltpu.VMEM((tokens, kvw), bf),
                pltpu.VMEM((piece, kvw), f32),
            ),
            in_specs=[pl.BlockSpec(memory_space=pl.ANY)] * 7,
            out_specs=(vmem, vmem, vmem),
            scratch_shapes=[
                pltpu.VMEM((tokens, normed_input.shape[2]), bf),
                pltpu.VMEM((tokens, queries.shape[2]), bf),
                pltpu.VMEM((tokens, kvw), bf),
                pltpu.VMEM((tokens, kvw), bf),
                pltpu.VMEM((tokens, queries.shape[2]), bf),
                pltpu.VMEM((tokens, queries.shape[2]), bf),
                pltpu.VMEM((1, tokens), jnp.int32),
                pltpu.VMEM((seq, hq * hw), bf),
                pltpu.VMEM((seq, hw), bf),
                pltpu.VMEM((seq, hw), bf),
                pltpu.VMEM((seq, hq * hw), bf),
                pltpu.VMEM((n, 8, tokens), f32),
                pltpu.VMEM((n, 8, tokens), f32),
                pltpu.VMEM((n * rows, tokens), bf),
                pltpu.VMEM((rows, seq), bf),
                pltpu.VMEM((seq, tokens), f32),
                pltpu.VMEM((seq, hw), f32),
                pltpu.VMEM((seq, hw), f32),
                pltpu.VMEM((n, tokens, hq * hw), bf),
                pltpu.VMEM((n, tokens, hw), bf),
                pltpu.VMEM((copies, tokens, kvw), bf),
                pltpu.VMEM((copies, seq, kvw), bf),
                pltpu.VMEM((rows, width), f32),
                pltpu.VMEM((chips, ndp, piece, width), bf),
                pltpu.VMEM((chips, ndp, piece, width), bf),
                dma((7,)), dma((6,)), dma((6,)), dma((8,)), dma((2,)), dma((2,)),
                dma((4,)), dma((1,)), dma((chips // 2, n)), dma((chips // 2,)), dma((chips,)), dma((chips,)),
                pltpu.SemaphoreType.REGULAR((max(1, ndp - 2), 2)),
            ],
            compiler_params=pltpu.CompilerParams(
                collective_id=0, has_side_effects=True, vmem_limit_bytes=60 * 1024 * 1024
            ),
            name="attention_backward",
        )(normed_input[0], queries[0], keys[0], values[0], saved_output[0], cotangent[0], doc_ids)
        def finish(*refs):
            copies_out = [
                pltpu.make_async_copy(src, dst, refs[6].at[index])
                for index, (src, dst) in enumerate(zip(refs[:3], refs[3:6]))
            ]
            for copy in copies_out:
                copy.start()
            for copy in copies_out:
                copy.wait()

        anywhere = pl.BlockSpec(memory_space=pl.ANY)
        dq, dk, dw = pl.pallas_call(
            finish,
            out_shape=tuple(jax.ShapeDtypeStruct(part.shape, part.dtype) for part in (dq, dk, dw)),
            in_specs=[anywhere] * 3,
            out_specs=(anywhere,) * 3,
            scratch_shapes=[dma((3,))],
            name="finish",
        )(pltpu.with_memory_space_constraint(dq, pltpu.VMEM), pltpu.with_memory_space_constraint(dk, pltpu.VMEM), pltpu.with_memory_space_constraint(dw, pltpu.VMEM))
        return dq[None], dk[None], dw

    spec = P("dp", "seq", None)
    return jax.shard_map(
        local,
        mesh=mesh,
        in_specs=(spec,) * 6 + (P("dp", "seq"),),
        out_specs=(spec, spec, P(("seq", "dp"), None)),
        check_vma=False,
    )
```

```python
import functools

import jax
import jax.numpy as jnp
from jax import lax
from jax.experimental import pallas as pl
from jax.experimental.pallas import tpu as pltpu
from jax.sharding import PartitionSpec as P

QUERY_HEADS = 16
KEY_VALUE_HEADS = 8
HEAD_WIDTH = 128
CORES = 2
EARLY, MIDDLE = 2, 4
FIRST = 4
MESH = pl.DeviceIdType.MESH

query_scale = 144.0 ** (-0.5)
soft_cap = 50.0


def flip(index, mask, count):
    out, bit = 0, 1
    while bit < count:
        digit = lax.rem(index // bit, 2)
        out = out + (1 - digit if mask & bit else digit) * bit
        bit *= 2
    return out


def at(index, width):
    start = index * width
    return pl.ds(start if isinstance(index, int) else pl.multiple_of(start, width), width)


def nt(a, b):
    return lax.dot_general(a, b, (((1,), (1,)), ((), ())), preferred_element_type=jnp.float32)


def tn(a, b):
    return lax.dot_general(a, b, (((0,), (0,)), ((), ())), preferred_element_type=jnp.float32)


def kernel(
    n, ndp, total_tokens,
    x_in, q_in, k_in, v_in, o_in, do_in, doc_in,
    dq_out, dk_out, dw_out,
    x_ref, q_ref, k_ref, v_ref, o_ref, do_ref, doc_ref,
    rq, rk, rv, rdo, meta, rmeta, xt, rx, dock,
    dk_acc, dv_acc, kept_t, kept_w, kept_i, dqs, dks, rdk, vg, pf, zs, zr,
    load_sem, in_send, in_recv, local_sem, out_send, out_recv, vg_send, near_recv, vg_recv,
    relay_recv, fwd_recv, z_recv, dp_sem,
):
    me = lax.axis_index("seq")
    dme = lax.axis_index("dp")
    tokens = q_ref.shape[0]
    seq = n * tokens
    hw = HEAD_WIDTH
    group = QUERY_HEADS // KEY_VALUE_HEADS
    hq = QUERY_HEADS // n
    copies = group // hq
    rows = x_ref.shape[1] // n
    piece = rows // ndp
    chips = n // CORES
    width = CORES * hw // copies
    reach = (seq // 2 - 1 + tokens - 1) // tokens
    chip, core = me // CORES, lax.rem(me, CORES)
    partner = chip * CORES + (1 - core)

    below, above = dme > 0, dme < ndp - 1
    barrier = pltpu.get_barrier_semaphore()
    for off in range(n - 1, 0, -1):
        pl.semaphore_signal(barrier, inc=1, device_id={"seq": flip(me, off, n)}, device_id_type=MESH)

    def tell_dp(up, down):
        @pl.when(above)
        def _():
            pl.semaphore_signal(up, inc=1, device_id={"dp": dme + 1}, device_id_type=MESH)

        @pl.when(below)
        def _():
            pl.semaphore_signal(down, inc=1, device_id={"dp": dme - 1}, device_id_type=MESH)

    tell_dp(barrier, barrier)

    loads = [
        pltpu.make_async_copy(src, dst, load_sem.at[index])
        for index, (src, dst) in enumerate((
            (do_in, do_ref), (o_in, o_ref), (doc_in, doc_ref), (x_in, x_ref),
            (k_in, k_ref), (v_in, v_ref), (q_in, q_ref),
        ))
    ]
    for load in loads:
        load.start()

    def inputs(dest, slot, local=False):
        kv = dest * hq // group
        sources = (k_in, v_in, q_in, do_in) if local else (k_ref, v_ref, q_ref, do_ref)
        return [
            (sources[0].at[:, at(kv, hw)], rk.at[at(slot, tokens), :]),
            (sources[1].at[:, at(kv, hw)], rv.at[at(slot, tokens), :]),
            (sources[2].at[:, at(dest, hq * hw)], rq.at[at(slot, tokens), :]),
            (sources[3].at[:, at(dest, hq * hw)], rdo.at[at(slot, tokens), :]),
            (meta.at[dest], rmeta.at[slot]),
            (xt.at[at(dest, rows), :], rx.at[:, at(slot, tokens)]),
        ]

    def input_copy(kind, off):
        peer = flip(me, off, n)
        src, dst = inputs(peer, me)[kind]
        return pltpu.make_async_remote_copy(
            src_ref=src, dst_ref=dst, send_sem=in_send.at[kind], recv_sem=in_recv.at[kind],
            device_id={"seq": peer}, device_id_type=MESH,
        )

    def own_copy(kind):
        src, dst = inputs(me, me, True)[kind]
        return pltpu.make_async_copy(src, dst, local_sem.at[kind])

    def bulk(ref, sem):
        return pltpu.make_async_remote_copy(
            src_ref=ref, dst_ref=ref, send_sem=sem, recv_sem=sem,
            device_id={"seq": partner}, device_id_type=MESH,
        )

    rest = pl.ds(0, (n - 1) * tokens)
    others = [
        rk.at[rest, :], rv.at[rest, :], rq.at[rest, :], rdo.at[rest, :], rmeta.at[pl.ds(0, n - 1)],
        xt.at[pl.ds(0, (n - 1) * rows), :],
    ]

    for kind in range(4):
        own_copy(kind).start()
    for load in loads[:3]:
        load.wait()
    docs = doc_ref[...].astype(jnp.float32)
    for head in range(QUERY_HEADS):
        span = slice(head * hw, (head + 1) * hw)
        prod = do_ref[:, span].astype(jnp.float32) * o_ref[:, span].astype(jnp.float32)
        meta[head // hq, head % hq : head % hq + 1, :] = jnp.sum(prod.T, axis=0, keepdims=True)
    for dest in range(n):
        meta[dest, hq : hq + 1, :] = docs
        if hq + 1 < meta.shape[1]:
            meta[dest, hq + 1 :, :] = jnp.zeros((meta.shape[1] - hq - 1, tokens), jnp.float32)
    loads[3].wait()
    for c in range(x_ref.shape[1] // hw):
        span = slice(c * hw, (c + 1) * hw)
        xt[span, :] = x_ref[:, span].astype(jnp.float32).T.astype(jnp.bfloat16)
    for load in loads[4:]:
        load.wait()
    pl.semaphore_wait(barrier, n - 1 + below.astype(jnp.int32) + above.astype(jnp.int32))

    order = list(range(n - 1, 0, -1))
    for off in order:
        for kind in range(5):
            input_copy(kind, off).start()
    for off in order:
        input_copy(5, off).start()
    own_copy(4).start()
    own_copy(5).start()

    for step in range(ndp - 2):
        tell_dp(dp_sem.at[step, 0], dp_sem.at[step, 1])

        @pl.when(below)
        def _():
            pl.semaphore_wait(dp_sem.at[step, 0], 1)

        @pl.when(above)
        def _():
            pl.semaphore_wait(dp_sem.at[step, 1], 1)

    for kind in range(5):
        own_copy(kind).wait()
    for kind in range(5):
        bulk(others[kind], in_recv.at[kind]).wait_recv()

    def dk_slot(source):
        if copies == 1:
            return dk_out.at[:, at(source, hw)]
        return rdk.at[lax.rem(source, copies), :, at(source // copies, hw)]

    def dq_copy(off):
        peer = flip(me, off, n)
        return pltpu.make_async_remote_copy(
            src_ref=dqs.at[peer], dst_ref=dq_out.at[:, at(me, hq * hw)],
            send_sem=out_send.at[0], recv_sem=out_recv.at[0],
            device_id={"seq": peer}, device_id_type=MESH,
        )

    def dk_copy(off):
        peer = flip(me, off, n)
        return pltpu.make_async_remote_copy(
            src_ref=dks.at[peer], dst_ref=dk_slot(me),
            send_sem=out_send.at[1], recv_sem=out_recv.at[1],
            device_id={"seq": peer}, device_id_type=MESH,
        )

    def dq_local():
        return pltpu.make_async_copy(dqs.at[me], dq_out.at[:, at(me, hq * hw)], local_sem.at[6])

    def dk_local():
        return pltpu.make_async_copy(dks.at[me], dk_slot(me), local_sem.at[7])

    def vg_slot(source, i):
        return vg.at[lax.rem(source, copies), at(i, tokens), at(source // copies, hw)]

    def chip_peer(c):
        return partner if c == 0 else flip(chip, c, chips) * CORES + core

    def vg_arrival(c, i):
        return near_recv.at[0] if c == 0 else vg_recv.at[c // 2, i]

    def vg_copy(c, i):
        return pltpu.make_async_remote_copy(
            src_ref=vg_slot(me, i), dst_ref=vg_slot(me, i),
            send_sem=vg_send.at[0], recv_sem=vg_arrival(c, i),
            device_id={"seq": chip_peer(c)}, device_id_type=MESH,
        )

    direct = [c for c in range(chips) if c < 2 or c % 2 == 0]
    evens = [c for c in direct if c > 1]

    def relay_copy(c, half, i):
        source, target = (1, c - 1) if half == 0 else (c - 1, 1)
        start = i * tokens + half * (tokens // 2)
        origin = chip_peer(source)
        slot = vg.at[lax.rem(origin, copies), at(start // (tokens // 2), tokens // 2), at(origin // copies, hw)]
        return pltpu.make_async_remote_copy(
            src_ref=slot, dst_ref=slot,
            send_sem=vg_send.at[1], recv_sem=relay_recv.at[c // 2],
            device_id={"seq": chip_peer(target)}, device_id_type=MESH,
        )

    def fwd_slot(source):
        return vg.at[lax.rem(source, copies), :, at(source // copies, hw)]

    def fwd_copy(c, source):
        return pltpu.make_async_remote_copy(
            src_ref=fwd_slot(source), dst_ref=fwd_slot(source),
            send_sem=vg_send.at[2], recv_sem=fwd_recv.at[c],
            device_id={"seq": partner}, device_id_type=MESH,
        )

    for j in range(n):
        dock[at(j, tokens), :] = jnp.broadcast_to(rmeta[j, hq : hq + 1, :], (tokens, tokens)).T

    causal = lax.broadcasted_iota(jnp.int32, (tokens, tokens), 0) <= lax.broadcasted_iota(
        jnp.int32, (tokens, tokens), 1
    )
    def stacked(ref, i):
        return jnp.concatenate([ref[at(i, tokens), g * hw : (g + 1) * hw] for g in range(hq)], axis=0)

    windows = [range(max(0, i - reach), i + 1) for i in range(n)]
    pairs = {pair: slot for slot, pair in enumerate((i, j) for i in range(n) for j in windows[i])}

    for i in reversed(range(n)):
        here = at(i, tokens)
        q2, do2 = stacked(rq, i), stacked(rdo, i)
        docq = rmeta[i, hq : hq + 1, :]
        totals = jnp.zeros((1, hq * tokens), jnp.float32)
        for j in windows[i]:
            t = jnp.tanh(nt(rk[at(j, tokens), :], q2) * (query_scale / soft_cap))
            allowed = dock[at(j, tokens), :] == docq
            if i == j:
                allowed = allowed & causal
            mask = jnp.where(allowed, 1.0, 0.0)
            w = jnp.exp(soft_cap * t) * jnp.concatenate([mask] * hq, axis=1)
            totals = totals + jnp.sum(w, axis=0, keepdims=True)
            kept_t[pairs[i, j]] = t
            kept_w[pairs[i, j]] = w
        inverse = 1.0 / totals
        kept_i[i] = inverse
        for j in windows[i]:
            p16 = (kept_w[pairs[i, j]] * inverse).astype(jnp.bfloat16)
            dv_term = jnp.dot(p16, do2, preferred_element_type=jnp.float32)
            if i == min(n - 1, j + reach):
                dv_acc[at(j, tokens), :] = dv_term
            else:
                dv_acc[at(j, tokens), :] += dv_term
        vg[lax.rem(me, copies), at(i, tokens), at(me // copies, hw)] = dv_acc[here, :].astype(jnp.bfloat16)
        for c in reversed(direct):
            vg_copy(c, i).start()

    def scores_back(i):
        q2, do2 = stacked(rq, i), stacked(rdo, i)
        delta = jnp.concatenate([rmeta[i, g : g + 1, :] for g in range(hq)], axis=1)
        dq = jnp.zeros((hq * tokens, hw), jnp.float32)
        for j in windows[i]:
            t = kept_t[pairs[i, j]]
            p = kept_w[pairs[i, j]] * kept_i[i]
            ds = p * (nt(rv[at(j, tokens), :], do2) - delta) * ((1.0 - t * t) * query_scale)
            ds16 = ds.astype(jnp.bfloat16)
            dk_term = jnp.dot(ds16, q2, preferred_element_type=jnp.float32)
            if i == min(n - 1, j + reach):
                dk_acc[at(j, tokens), :] = dk_term
            else:
                dk_acc[at(j, tokens), :] += dk_term
            dq = dq + tn(ds16, rk[at(j, tokens), :])
        for g in range(hq):
            dqs[i, :, g * hw : (g + 1) * hw] = dq[g * tokens : (g + 1) * tokens].astype(jnp.bfloat16)
        dks[i] = dk_acc[at(i, tokens), :].astype(jnp.bfloat16)

    def out_start(off):
        dq_copy(off).start()
        dk_copy(off).start()

    outgoing = list(range(3, n, 2)) + list(range(2, n, 2)) + [1]

    def z_copy(c, off):
        dest = lax.rem(dme + off, ndp)
        return pltpu.make_async_remote_copy(
            src_ref=zs.at[c, dest], dst_ref=zr.at[c, dme],
            send_sem=vg_send.at[3], recv_sem=z_recv.at[c],
            device_id={"dp": dest}, device_id_type=MESH,
        )

    def weight_term(c):
        columns = at(flip(chip, c, chips), width)
        values = vg[0, :, columns]
        if copies > 1:
            values = values.astype(jnp.float32)
            for other in range(1, copies):
                values = values + vg[other, :, columns].astype(jnp.float32)
            values = values.astype(jnp.bfloat16)
        pf[...] = jnp.dot(rx[...], values, preferred_element_type=jnp.float32)
        for d in range(ndp):
            zs[c, d] = pf[d * piece : (d + 1) * piece, :].astype(jnp.bfloat16)
        for off in range(1, ndp):
            z_copy(c, off).start()

    for i in reversed(range(n)):
        scores_back(i)
        if i == FIRST:
            own_copy(5).wait()
            bulk(others[5], in_recv.at[5]).wait_recv()
            bulk(fwd_slot(partner), near_recv.at[0]).wait_recv()
            weight_term(0)
    dq_local().start()
    dk_local().start()
    for i in reversed(range(n)):
        if chips > 1:
            bulk(vg_slot(chip_peer(1), i), vg_arrival(1, i)).wait_recv()
        for c in evens:
            if c + 1 < chips:
                relay_copy(c + 1, 0, i).start()
        for c in evens:
            bulk(vg_slot(chip_peer(c), i), vg_arrival(c, i)).wait_recv()
            if c + 1 < chips:
                relay_copy(c + 1, 1, i).start()
        if i == n // 2:
            for off in outgoing[:EARLY]:
                out_start(off)
    for c in direct:
        if c:
            fwd_copy(c, chip_peer(c)).start()
    for off in outgoing[EARLY:MIDDLE]:
        out_start(off)
    for c in direct:
        if c:
            bulk(fwd_slot(flip(chip, c, chips) * CORES + (1 - core)), fwd_recv.at[c]).wait_recv()
            weight_term(c)
    relayed = [c for c in range(chips) if c not in direct]
    for c in relayed:
        bulk(fwd_slot(chip_peer(c)), relay_recv.at[c // 2]).wait_recv()
        fwd_copy(c, chip_peer(c)).start()
    for off in outgoing[MIDDLE:]:
        out_start(off)
    for c in relayed:
        bulk(fwd_slot(flip(chip, c, chips) * CORES + (1 - core)), fwd_recv.at[c]).wait_recv()
        weight_term(c)

    for c in direct + relayed:
        value = zs[c, dme].astype(jnp.float32)
        bulk(zr.at[c, pl.ds(0, ndp - 1)], z_recv.at[c]).wait_recv()
        for off in range(1, ndp):
            value = value + zr[c, lax.rem(dme + ndp - off, ndp)].astype(jnp.float32)
        dw_out[:, at(flip(chip, c, chips), width)] = value * total_tokens ** (-0.5)

    for index, ref in enumerate((dqs, dks)):
        bulk(ref.at[pl.ds(0, n - 1)], out_recv.at[index]).wait_recv()
    dq_local().wait()
    dk_local().wait()

    if copies > 1:
        total = rdk[0].astype(jnp.float32)
        for other in range(1, copies):
            total = total + rdk[other].astype(jnp.float32)
        dk_out[...] = total.astype(jnp.bfloat16)

    for kind in range(6):
        bulk(others[kind], in_send.at[kind]).wait_send()
    for index, ref in enumerate((dqs, dks)):
        bulk(ref.at[pl.ds(0, n - 1)], out_send.at[index]).wait_send()
    for index, count in enumerate((len(direct), len(relayed), chips - 1)):
        if count:
            bulk(vg.at[0, :, pl.ds(0, count * hw)], vg_send.at[index]).wait_send()
    bulk(zs.at[:, pl.ds(0, ndp - 1)], vg_send.at[3]).wait_send()


def solution(mesh):
    n, ndp = mesh.shape["seq"], mesh.shape["dp"]

    def local(normed_input, queries, keys, values, saved_output, cotangent, doc_ids):
        tokens = queries.shape[1]
        seq = n * tokens
        hw = HEAD_WIDTH
        hq = QUERY_HEADS // n
        copies = QUERY_HEADS // KEY_VALUE_HEADS // hq
        kvw = keys.shape[2]
        rows = normed_input.shape[2] // n
        piece = rows // ndp
        chips = n // CORES
        width = CORES * hw // copies
        reach = (seq // 2 - 1 + tokens - 1) // tokens
        pairs = sum(min(i, reach) + 1 for i in range(n))
        bf, f32 = jnp.bfloat16, jnp.float32
        dma = pltpu.SemaphoreType.DMA
        vmem = pl.BlockSpec(memory_space=pltpu.VMEM)
        dq, dk, dw = pl.pallas_call(
            functools.partial(kernel, n, ndp, float(ndp * seq)),
            out_shape=(
                pltpu.VMEM((tokens, queries.shape[2]), bf),
                pltpu.VMEM((tokens, kvw), bf),
                pltpu.VMEM((piece, kvw), f32),
            ),
            in_specs=[pl.BlockSpec(memory_space=pl.ANY)] * 7,
            out_specs=(vmem, vmem, vmem),
            scratch_shapes=[
                pltpu.VMEM((tokens, normed_input.shape[2]), bf),
                pltpu.VMEM((tokens, queries.shape[2]), bf),
                pltpu.VMEM((tokens, kvw), bf),
                pltpu.VMEM((tokens, kvw), bf),
                pltpu.VMEM((tokens, queries.shape[2]), bf),
                pltpu.VMEM((tokens, queries.shape[2]), bf),
                pltpu.VMEM((1, tokens), jnp.int32),
                pltpu.VMEM((seq, hq * hw), bf),
                pltpu.VMEM((seq, hw), bf),
                pltpu.VMEM((seq, hw), bf),
                pltpu.VMEM((seq, hq * hw), bf),
                pltpu.VMEM((n, 8, tokens), f32),
                pltpu.VMEM((n, 8, tokens), f32),
                pltpu.VMEM((n * rows, tokens), bf),
                pltpu.VMEM((rows, seq), bf),
                pltpu.VMEM((seq, tokens), f32),
                pltpu.VMEM((seq, hw), f32),
                pltpu.VMEM((seq, hw), f32),
                pltpu.VMEM((pairs, tokens, hq * tokens), f32),
                pltpu.VMEM((pairs, tokens, hq * tokens), f32),
                pltpu.VMEM((n, 1, hq * tokens), f32),
                pltpu.VMEM((n, tokens, hq * hw), bf),
                pltpu.VMEM((n, tokens, hw), bf),
                pltpu.VMEM((copies, tokens, kvw), bf),
                pltpu.VMEM((copies, seq, kvw), bf),
                pltpu.VMEM((rows, width), f32),
                pltpu.VMEM((chips, ndp, piece, width), bf),
                pltpu.VMEM((chips, ndp, piece, width), bf),
                dma((7,)), dma((6,)), dma((6,)), dma((8,)), dma((2,)), dma((2,)),
                dma((4,)), dma((1,)), dma((chips // 2, n)), dma((chips // 2,)), dma((chips,)), dma((chips,)),
                pltpu.SemaphoreType.REGULAR((max(1, ndp - 2), 2)),
            ],
            compiler_params=pltpu.CompilerParams(
                collective_id=0, has_side_effects=True, vmem_limit_bytes=60 * 1024 * 1024
            ),
            name="attention_backward",
        )(normed_input[0], queries[0], keys[0], values[0], saved_output[0], cotangent[0], doc_ids)
        def finish(*refs):
            copies_out = [
                pltpu.make_async_copy(src, dst, refs[6].at[index])
                for index, (src, dst) in enumerate(zip(refs[:3], refs[3:6]))
            ]
            for copy in copies_out:
                copy.start()
            for copy in copies_out:
                copy.wait()

        anywhere = pl.BlockSpec(memory_space=pl.ANY)
        dq, dk, dw = pl.pallas_call(
            finish,
            out_shape=tuple(jax.ShapeDtypeStruct(part.shape, part.dtype) for part in (dq, dk, dw)),
            in_specs=[anywhere] * 3,
            out_specs=(anywhere,) * 3,
            scratch_shapes=[dma((3,))],
            name="finish",
        )(pltpu.with_memory_space_constraint(dq, pltpu.VMEM), pltpu.with_memory_space_constraint(dk, pltpu.VMEM), pltpu.with_memory_space_constraint(dw, pltpu.VMEM))
        return dq[None], dk[None], dw

    spec = P("dp", "seq", None)
    return jax.shard_map(
        local,
        mesh=mesh,
        in_specs=(spec,) * 6 + (P("dp", "seq"),),
        out_specs=(spec, spec, P(("seq", "dp"), None)),
        check_vma=False,
    )
```

```python
import functools

import jax
import jax.numpy as jnp
from jax import lax
from jax.experimental import pallas as pl
from jax.experimental.pallas import tpu as pltpu
from jax.sharding import PartitionSpec as P

QUERY_HEADS = 16
KEY_VALUE_HEADS = 8
HEAD_WIDTH = 128
CORES = 2
EARLY, MIDDLE = 2, 4
FIRST = 4
MESH = pl.DeviceIdType.MESH

query_scale = 144.0 ** (-0.5)
soft_cap = 50.0
LOG2E = 1.4426950408889634


def flip(index, mask, count):
    out, bit = 0, 1
    while bit < count:
        digit = lax.rem(index // bit, 2)
        out = out + (1 - digit if mask & bit else digit) * bit
        bit *= 2
    return out


def at(index, width):
    start = index * width
    return pl.ds(start if isinstance(index, int) else pl.multiple_of(start, width), width)


def nt(a, b):
    return lax.dot_general(a, b, (((1,), (1,)), ((), ())), preferred_element_type=jnp.float32)


def tn(a, b):
    return lax.dot_general(a, b, (((0,), (0,)), ((), ())), preferred_element_type=jnp.float32)


def kernel(
    n, ndp, total_tokens,
    x_in, q_in, k_in, v_in, o_in, do_in, doc_in,
    dq_out, dk_out, dw_out,
    x_ref, q_ref, k_ref, v_ref, o_ref, do_ref, doc_ref,
    rq, rk, rv, rdo, meta, rmeta, xt, rx, dock,
    dk_acc, dv_acc, kept_t, kept_w, kept_i, dqs, dks, rdk, vg, pf, zs, zr,
    load_sem, in_send, in_recv, local_sem, out_send, out_recv, vg_send, near_recv, vg_recv,
    relay_recv, fwd_recv, z_recv, dp_sem,
):
    me = lax.axis_index("seq")
    dme = lax.axis_index("dp")
    tokens = q_ref.shape[0]
    seq = n * tokens
    hw = HEAD_WIDTH
    group = QUERY_HEADS // KEY_VALUE_HEADS
    hq = QUERY_HEADS // n
    copies = group // hq
    rows = x_ref.shape[1] // n
    piece = rows // ndp
    chips = n // CORES
    width = CORES * hw // copies
    reach = (seq // 2 - 1 + tokens - 1) // tokens
    chip, core = me // CORES, lax.rem(me, CORES)
    partner = chip * CORES + (1 - core)

    below, above = dme > 0, dme < ndp - 1
    barrier = pltpu.get_barrier_semaphore()
    for off in range(n - 1, 0, -1):
        pl.semaphore_signal(barrier, inc=1, device_id={"seq": flip(me, off, n)}, device_id_type=MESH)

    def tell_dp(up, down):
        @pl.when(above)
        def _():
            pl.semaphore_signal(up, inc=1, device_id={"dp": dme + 1}, device_id_type=MESH)

        @pl.when(below)
        def _():
            pl.semaphore_signal(down, inc=1, device_id={"dp": dme - 1}, device_id_type=MESH)

    tell_dp(barrier, barrier)

    loads = [
        pltpu.make_async_copy(src, dst, load_sem.at[index])
        for index, (src, dst) in enumerate((
            (do_in, do_ref), (o_in, o_ref), (doc_in, doc_ref), (x_in, x_ref),
            (k_in, k_ref), (v_in, v_ref), (q_in, q_ref),
        ))
    ]
    for load in loads:
        load.start()

    def inputs(dest, slot, local=False):
        kv = dest * hq // group
        sources = (k_in, v_in, q_in, do_in) if local else (k_ref, v_ref, q_ref, do_ref)
        return [
            (sources[0].at[:, at(kv, hw)], rk.at[at(slot, tokens), :]),
            (sources[1].at[:, at(kv, hw)], rv.at[at(slot, tokens), :]),
            (sources[2].at[:, at(dest, hq * hw)], rq.at[at(slot, tokens), :]),
            (sources[3].at[:, at(dest, hq * hw)], rdo.at[at(slot, tokens), :]),
            (meta.at[dest], rmeta.at[slot]),
            (xt.at[at(dest, rows), :], rx.at[:, at(slot, tokens)]),
        ]

    def input_copy(kind, off):
        peer = flip(me, off, n)
        src, dst = inputs(peer, me)[kind]
        return pltpu.make_async_remote_copy(
            src_ref=src, dst_ref=dst, send_sem=in_send.at[kind], recv_sem=in_recv.at[kind],
            device_id={"seq": peer}, device_id_type=MESH,
        )

    def own_copy(kind):
        src, dst = inputs(me, me, True)[kind]
        return pltpu.make_async_copy(src, dst, local_sem.at[kind])

    def bulk(ref, sem):
        return pltpu.make_async_remote_copy(
            src_ref=ref, dst_ref=ref, send_sem=sem, recv_sem=sem,
            device_id={"seq": partner}, device_id_type=MESH,
        )

    rest = pl.ds(0, (n - 1) * tokens)
    others = [
        rk.at[rest, :], rv.at[rest, :], rq.at[rest, :], rdo.at[rest, :], rmeta.at[pl.ds(0, n - 1)],
        xt.at[pl.ds(0, (n - 1) * rows), :],
    ]

    for kind in range(4):
        own_copy(kind).start()
    for load in loads[:3]:
        load.wait()
    docs = doc_ref[...].astype(jnp.float32)
    for head in range(QUERY_HEADS):
        span = slice(head * hw, (head + 1) * hw)
        prod = do_ref[:, span].astype(jnp.float32) * o_ref[:, span].astype(jnp.float32)
        meta[head // hq, head % hq : head % hq + 1, :] = jnp.sum(prod.T, axis=0, keepdims=True)
    for dest in range(n):
        meta[dest, hq : hq + 1, :] = docs
        if hq + 1 < meta.shape[1]:
            meta[dest, hq + 1 :, :] = jnp.zeros((meta.shape[1] - hq - 1, tokens), jnp.float32)
    loads[3].wait()
    for c in range(x_ref.shape[1] // hw):
        span = slice(c * hw, (c + 1) * hw)
        xt[span, :] = x_ref[:, span].astype(jnp.float32).T.astype(jnp.bfloat16)
    for load in loads[4:]:
        load.wait()
    pl.semaphore_wait(barrier, n - 1 + below.astype(jnp.int32) + above.astype(jnp.int32))

    order = list(range(n - 1, 0, -1))
    for off in order:
        for kind in range(5):
            input_copy(kind, off).start()
    for off in order:
        input_copy(5, off).start()
    own_copy(4).start()
    own_copy(5).start()

    for step in range(ndp - 2):
        tell_dp(dp_sem.at[step, 0], dp_sem.at[step, 1])

        @pl.when(below)
        def _():
            pl.semaphore_wait(dp_sem.at[step, 0], 1)

        @pl.when(above)
        def _():
            pl.semaphore_wait(dp_sem.at[step, 1], 1)

    for kind in range(5):
        own_copy(kind).wait()
    for kind in range(5):
        bulk(others[kind], in_recv.at[kind]).wait_recv()

    def dk_slot(source):
        if copies == 1:
            return dk_out.at[:, at(source, hw)]
        return rdk.at[lax.rem(source, copies), :, at(source // copies, hw)]

    def dq_copy(off):
        peer = flip(me, off, n)
        return pltpu.make_async_remote_copy(
            src_ref=dqs.at[peer], dst_ref=dq_out.at[:, at(me, hq * hw)],
            send_sem=out_send.at[0], recv_sem=out_recv.at[0],
            device_id={"seq": peer}, device_id_type=MESH,
        )

    def dk_copy(off):
        peer = flip(me, off, n)
        return pltpu.make_async_remote_copy(
            src_ref=dks.at[peer], dst_ref=dk_slot(me),
            send_sem=out_send.at[1], recv_sem=out_recv.at[1],
            device_id={"seq": peer}, device_id_type=MESH,
        )

    def dq_local():
        return pltpu.make_async_copy(dqs.at[me], dq_out.at[:, at(me, hq * hw)], local_sem.at[6])

    def dk_local():
        return pltpu.make_async_copy(dks.at[me], dk_slot(me), local_sem.at[7])

    def vg_slot(source, i):
        return vg.at[lax.rem(source, copies), at(i, tokens), at(source // copies, hw)]

    def chip_peer(c):
        return partner if c == 0 else flip(chip, c, chips) * CORES + core

    def vg_arrival(c, i):
        return near_recv.at[0] if c == 0 else vg_recv.at[c // 2, i]

    def vg_copy(c, i):
        return pltpu.make_async_remote_copy(
            src_ref=vg_slot(me, i), dst_ref=vg_slot(me, i),
            send_sem=vg_send.at[0], recv_sem=vg_arrival(c, i),
            device_id={"seq": chip_peer(c)}, device_id_type=MESH,
        )

    direct = [c for c in range(chips) if c < 2 or c % 2 == 0]
    evens = [c for c in direct if c > 1]

    def relay_copy(c, half, i):
        source, target = (1, c - 1) if half == 0 else (c - 1, 1)
        start = i * tokens + half * (tokens // 2)
        origin = chip_peer(source)
        slot = vg.at[lax.rem(origin, copies), at(start // (tokens // 2), tokens // 2), at(origin // copies, hw)]
        return pltpu.make_async_remote_copy(
            src_ref=slot, dst_ref=slot,
            send_sem=vg_send.at[1], recv_sem=relay_recv.at[c // 2],
            device_id={"seq": chip_peer(target)}, device_id_type=MESH,
        )

    def fwd_slot(source):
        return vg.at[lax.rem(source, copies), :, at(source // copies, hw)]

    def fwd_copy(c, source):
        return pltpu.make_async_remote_copy(
            src_ref=fwd_slot(source), dst_ref=fwd_slot(source),
            send_sem=vg_send.at[2], recv_sem=fwd_recv.at[c],
            device_id={"seq": partner}, device_id_type=MESH,
        )

    for j in range(n):
        dock[at(j, tokens), :] = jnp.broadcast_to(rmeta[j, hq : hq + 1, :], (tokens, tokens)).T

    causal = lax.broadcasted_iota(jnp.int32, (tokens, tokens), 0) <= lax.broadcasted_iota(
        jnp.int32, (tokens, tokens), 1
    )
    def stacked(ref, i):
        return jnp.concatenate([ref[at(i, tokens), g * hw : (g + 1) * hw] for g in range(hq)], axis=0)

    windows = [range(max(0, i - reach), i + 1) for i in range(n)]
    pairs = {pair: slot for slot, pair in enumerate((i, j) for i in range(n) for j in windows[i])}

    for i in reversed(range(n)):
        here = at(i, tokens)
        q2, do2 = stacked(rq, i), stacked(rdo, i)
        docq = rmeta[i, hq : hq + 1, :]
        totals = jnp.zeros((1, hq * tokens), jnp.float32)
        for j in windows[i]:
            t = jnp.tanh(nt(rk[at(j, tokens), :], q2) * (query_scale / soft_cap))
            allowed = dock[at(j, tokens), :] == docq
            if i == j:
                allowed = allowed & causal
            mask = jnp.where(allowed, 1.0, 0.0)
            w = jnp.exp2((soft_cap * LOG2E) * t) * jnp.concatenate([mask] * hq, axis=1)
            totals = totals + jnp.sum(w, axis=0, keepdims=True)
            kept_t[pairs[i, j]] = t
            kept_w[pairs[i, j]] = w
        inverse = 1.0 / totals
        kept_i[i] = inverse
        for j in windows[i]:
            p16 = (kept_w[pairs[i, j]] * inverse).astype(jnp.bfloat16)
            dv_term = jnp.dot(p16, do2, preferred_element_type=jnp.float32)
            if i == min(n - 1, j + reach):
                dv_acc[at(j, tokens), :] = dv_term
            else:
                dv_acc[at(j, tokens), :] += dv_term
        vg[lax.rem(me, copies), at(i, tokens), at(me // copies, hw)] = dv_acc[here, :].astype(jnp.bfloat16)
        for c in reversed(direct):
            vg_copy(c, i).start()

    def scores_back(i):
        q2, do2 = stacked(rq, i), stacked(rdo, i)
        delta = jnp.concatenate([rmeta[i, g : g + 1, :] for g in range(hq)], axis=1)
        dq = jnp.zeros((hq * tokens, hw), jnp.float32)
        for j in windows[i]:
            t = kept_t[pairs[i, j]]
            p = kept_w[pairs[i, j]] * kept_i[i]
            ds = p * (nt(rv[at(j, tokens), :], do2) - delta) * (1.0 - t * t)
            ds16 = ds.astype(jnp.bfloat16)
            dk_term = jnp.dot(ds16, q2, preferred_element_type=jnp.float32)
            if i == min(n - 1, j + reach):
                dk_acc[at(j, tokens), :] = dk_term
            else:
                dk_acc[at(j, tokens), :] += dk_term
            dq = dq + tn(ds16, rk[at(j, tokens), :])
        for g in range(hq):
            dqs[i, :, g * hw : (g + 1) * hw] = (dq[g * tokens : (g + 1) * tokens] * query_scale).astype(jnp.bfloat16)
        dks[i] = (dk_acc[at(i, tokens), :] * query_scale).astype(jnp.bfloat16)

    def out_start(off):
        dq_copy(off).start()
        dk_copy(off).start()

    outgoing = list(range(3, n, 2)) + list(range(2, n, 2)) + [1]

    def z_copy(c, off):
        dest = lax.rem(dme + off, ndp)
        return pltpu.make_async_remote_copy(
            src_ref=zs.at[c, dest], dst_ref=zr.at[c, dme],
            send_sem=vg_send.at[3], recv_sem=z_recv.at[c],
            device_id={"dp": dest}, device_id_type=MESH,
        )

    def weight_term(c):
        columns = at(flip(chip, c, chips), width)
        values = vg[0, :, columns]
        if copies > 1:
            values = values.astype(jnp.float32)
            for other in range(1, copies):
                values = values + vg[other, :, columns].astype(jnp.float32)
            values = values.astype(jnp.bfloat16)
        pf[...] = jnp.dot(rx[...], values, preferred_element_type=jnp.float32)
        for d in range(ndp):
            zs[c, d] = pf[d * piece : (d + 1) * piece, :].astype(jnp.bfloat16)
        for off in range(1, ndp):
            z_copy(c, off).start()

    for i in reversed(range(n)):
        scores_back(i)
        if i == FIRST:
            own_copy(5).wait()
            bulk(others[5], in_recv.at[5]).wait_recv()
            bulk(fwd_slot(partner), near_recv.at[0]).wait_recv()
            weight_term(0)
    dq_local().start()
    dk_local().start()
    for i in reversed(range(n)):
        if chips > 1:
            bulk(vg_slot(chip_peer(1), i), vg_arrival(1, i)).wait_recv()
        for c in evens:
            if c + 1 < chips:
                relay_copy(c + 1, 0, i).start()
        for c in evens:
            bulk(vg_slot(chip_peer(c), i), vg_arrival(c, i)).wait_recv()
            if c + 1 < chips:
                relay_copy(c + 1, 1, i).start()
        if i == n // 2:
            for off in outgoing[:EARLY]:
                out_start(off)
    for c in direct:
        if c:
            fwd_copy(c, chip_peer(c)).start()
    for off in outgoing[EARLY:MIDDLE]:
        out_start(off)
    for c in direct:
        if c:
            bulk(fwd_slot(flip(chip, c, chips) * CORES + (1 - core)), fwd_recv.at[c]).wait_recv()
            weight_term(c)
    relayed = [c for c in range(chips) if c not in direct]
    for c in relayed:
        bulk(fwd_slot(chip_peer(c)), relay_recv.at[c // 2]).wait_recv()
        fwd_copy(c, chip_peer(c)).start()
    for off in outgoing[MIDDLE:]:
        out_start(off)
    for c in relayed:
        bulk(fwd_slot(flip(chip, c, chips) * CORES + (1 - core)), fwd_recv.at[c]).wait_recv()
        weight_term(c)

    for c in direct + relayed:
        value = zs[c, dme].astype(jnp.float32)
        bulk(zr.at[c, pl.ds(0, ndp - 1)], z_recv.at[c]).wait_recv()
        for off in range(1, ndp):
            value = value + zr[c, lax.rem(dme + ndp - off, ndp)].astype(jnp.float32)
        dw_out[:, at(flip(chip, c, chips), width)] = value * total_tokens ** (-0.5)

    for index, ref in enumerate((dqs, dks)):
        bulk(ref.at[pl.ds(0, n - 1)], out_recv.at[index]).wait_recv()
    dq_local().wait()
    dk_local().wait()

    if copies > 1:
        total = rdk[0].astype(jnp.float32)
        for other in range(1, copies):
            total = total + rdk[other].astype(jnp.float32)
        dk_out[...] = total.astype(jnp.bfloat16)

    for kind in range(6):
        bulk(others[kind], in_send.at[kind]).wait_send()
    for index, ref in enumerate((dqs, dks)):
        bulk(ref.at[pl.ds(0, n - 1)], out_send.at[index]).wait_send()
    for index, count in enumerate((len(direct), len(relayed), chips - 1)):
        if count:
            bulk(vg.at[0, :, pl.ds(0, count * hw)], vg_send.at[index]).wait_send()
    bulk(zs.at[:, pl.ds(0, ndp - 1)], vg_send.at[3]).wait_send()


def solution(mesh):
    n, ndp = mesh.shape["seq"], mesh.shape["dp"]

    def local(normed_input, queries, keys, values, saved_output, cotangent, doc_ids):
        tokens = queries.shape[1]
        seq = n * tokens
        hw = HEAD_WIDTH
        hq = QUERY_HEADS // n
        copies = QUERY_HEADS // KEY_VALUE_HEADS // hq
        kvw = keys.shape[2]
        rows = normed_input.shape[2] // n
        piece = rows // ndp
        chips = n // CORES
        width = CORES * hw // copies
        reach = (seq // 2 - 1 + tokens - 1) // tokens
        pairs = sum(min(i, reach) + 1 for i in range(n))
        bf, f32 = jnp.bfloat16, jnp.float32
        dma = pltpu.SemaphoreType.DMA
        vmem = pl.BlockSpec(memory_space=pltpu.VMEM)
        dq, dk, dw = pl.pallas_call(
            functools.partial(kernel, n, ndp, float(ndp * seq)),
            out_shape=(
                pltpu.VMEM((tokens, queries.shape[2]), bf),
                pltpu.VMEM((tokens, kvw), bf),
                pltpu.VMEM((piece, kvw), f32),
            ),
            in_specs=[pl.BlockSpec(memory_space=pl.ANY)] * 7,
            out_specs=(vmem, vmem, vmem),
            scratch_shapes=[
                pltpu.VMEM((tokens, normed_input.shape[2]), bf),
                pltpu.VMEM((tokens, queries.shape[2]), bf),
                pltpu.VMEM((tokens, kvw), bf),
                pltpu.VMEM((tokens, kvw), bf),
                pltpu.VMEM((tokens, queries.shape[2]), bf),
                pltpu.VMEM((tokens, queries.shape[2]), bf),
                pltpu.VMEM((1, tokens), jnp.int32),
                pltpu.VMEM((seq, hq * hw), bf),
                pltpu.VMEM((seq, hw), bf),
                pltpu.VMEM((seq, hw), bf),
                pltpu.VMEM((seq, hq * hw), bf),
                pltpu.VMEM((n, 8, tokens), f32),
                pltpu.VMEM((n, 8, tokens), f32),
                pltpu.VMEM((n * rows, tokens), bf),
                pltpu.VMEM((rows, seq), bf),
                pltpu.VMEM((seq, tokens), f32),
                pltpu.VMEM((seq, hw), f32),
                pltpu.VMEM((seq, hw), f32),
                pltpu.VMEM((pairs, tokens, hq * tokens), f32),
                pltpu.VMEM((pairs, tokens, hq * tokens), f32),
                pltpu.VMEM((n, 1, hq * tokens), f32),
                pltpu.VMEM((n, tokens, hq * hw), bf),
                pltpu.VMEM((n, tokens, hw), bf),
                pltpu.VMEM((copies, tokens, kvw), bf),
                pltpu.VMEM((copies, seq, kvw), bf),
                pltpu.VMEM((rows, width), f32),
                pltpu.VMEM((chips, ndp, piece, width), bf),
                pltpu.VMEM((chips, ndp, piece, width), bf),
                dma((7,)), dma((6,)), dma((6,)), dma((8,)), dma((2,)), dma((2,)),
                dma((4,)), dma((1,)), dma((chips // 2, n)), dma((chips // 2,)), dma((chips,)), dma((chips,)),
                pltpu.SemaphoreType.REGULAR((max(1, ndp - 2), 2)),
            ],
            compiler_params=pltpu.CompilerParams(
                collective_id=0, has_side_effects=True, vmem_limit_bytes=60 * 1024 * 1024
            ),
            name="attention_backward",
        )(normed_input[0], queries[0], keys[0], values[0], saved_output[0], cotangent[0], doc_ids)
        def finish(*refs):
            copies_out = [
                pltpu.make_async_copy(src, dst, refs[6].at[index])
                for index, (src, dst) in enumerate(zip(refs[:3], refs[3:6]))
            ]
            for copy in copies_out:
                copy.start()
            for copy in copies_out:
                copy.wait()

        anywhere = pl.BlockSpec(memory_space=pl.ANY)
        dq, dk, dw = pl.pallas_call(
            finish,
            out_shape=tuple(jax.ShapeDtypeStruct(part.shape, part.dtype) for part in (dq, dk, dw)),
            in_specs=[anywhere] * 3,
            out_specs=(anywhere,) * 3,
            scratch_shapes=[dma((3,))],
            name="finish",
        )(pltpu.with_memory_space_constraint(dq, pltpu.VMEM), pltpu.with_memory_space_constraint(dk, pltpu.VMEM), pltpu.with_memory_space_constraint(dw, pltpu.VMEM))
        return dq[None], dk[None], dw

    spec = P("dp", "seq", None)
    return jax.shard_map(
        local,
        mesh=mesh,
        in_specs=(spec,) * 6 + (P("dp", "seq"),),
        out_specs=(spec, spec, P(("seq", "dp"), None)),
        check_vma=False,
    )
```
